128 devices in a mesh: local: 16 (over z, y), data: 8 (over x, core).
Axes of the slice: x: 4, y: 4, z: 4, core: 2. Of those that a mesh axis runs over, the one named last changes fastest.
Arguments:
- tokens: bfloat16 [2, 16384, 2048], P(None, ('local', 'data'))
- cotangent: bfloat16 [2, 16384, 2048], P(None, ('local', 'data'))
- w_up: bfloat16 [2, 2048, 5632], P(None, ('local', 'data'))
- w_down: bfloat16 [2, 5632, 2048], P(None, ('local', 'data'))
Outputs:
- output 1: bfloat16 [2, 16384, 2048], P(None, ('local', 'data'))
- output 2: bfloat16 [2, 16384, 2048], P(None, ('local', 'data'))
- output 3: float32 [2, 2048, 5632], P(None, ('local', 'data'))
- output 4: float32 [2, 5632, 2048], P(None, ('local', 'data'))
All inputs are finite; a program needn't handle non-finite values.
Results may differ from the reference program's by a relative error of at most 0.0133437.
Values are sent between devices in bfloat16 or wider.
A program may use at most 1 GiB of HBM per device.

```python
import jax
import jax.numpy as jnp
from jax import lax

HIDDEN = 2048
FFN_WIDTH = 5632
TOKENS = 16384
LAYERS = 2
MICROBATCHES = 2
NORM_EPS = 1e-6


def setup_inputs(seed: int = 0) -> dict:
    key = jax.random.key(seed)
    key_x, key_g, key_up, key_down = jax.random.split(key, 4)
    tokens = jax.random.normal(key_x, (MICROBATCHES, TOKENS, HIDDEN), jnp.float32)
    cotangent = jax.random.normal(key_g, (MICROBATCHES, TOKENS, HIDDEN), jnp.float32)
    w_up = jax.random.normal(key_up, (LAYERS, HIDDEN, FFN_WIDTH), jnp.float32) * HIDDEN ** -0.5
    w_down = jax.random.normal(key_down, (LAYERS, FFN_WIDTH, HIDDEN), jnp.float32) * (1.5 * FFN_WIDTH ** -0.5)
    return {"tokens": tokens.astype(jnp.bfloat16), "cotangent": cotangent.astype(jnp.bfloat16), "w_up": w_up.astype(jnp.bfloat16), "w_down": w_down.astype(jnp.bfloat16)}


def norm_f32(x_f32):
    return x_f32 * lax.rsqrt(jnp.mean(x_f32 * x_f32, axis=-1, keepdims=True) + NORM_EPS)


def gelu_f32(pre_f32):
    return jax.nn.gelu(pre_f32, approximate=True)


def layer_forward(x_in, up_mat, down_mat):
    x_f32 = x_in.astype(jnp.float32)
    normed = norm_f32(x_f32).astype(jnp.bfloat16)
    pre_act = jnp.dot(normed, up_mat, preferred_element_type=jnp.float32).astype(jnp.bfloat16)
    hidden = gelu_f32(pre_act.astype(jnp.float32)).astype(jnp.bfloat16)
    x_out = (x_f32 + jnp.dot(hidden, down_mat, preferred_element_type=jnp.float32)).astype(jnp.bfloat16)
    return x_out, normed, pre_act, hidden


def layer_backward(d_out, x_in, normed, pre_act, hidden, up_mat, down_mat):
    d_hidden = jnp.dot(d_out, down_mat.T, preferred_element_type=jnp.float32)
    gelu_pull = jax.vjp(gelu_f32, pre_act.astype(jnp.float32))[1]
    d_pre = gelu_pull(d_hidden)[0].astype(jnp.bfloat16)
    d_normed = jnp.dot(d_pre, up_mat.T, preferred_element_type=jnp.float32)
    norm_pull = jax.vjp(norm_f32, x_in.astype(jnp.float32))[1]
    d_in = (d_out.astype(jnp.float32) + norm_pull(d_normed)[0]).astype(jnp.bfloat16)
    grad_up = jnp.dot(normed.T, d_pre, preferred_element_type=jnp.float32)
    grad_down = jnp.dot(hidden.T, d_out, preferred_element_type=jnp.float32)
    return d_in, grad_up, grad_down


def reference(tokens, cotangent, w_up, w_down):
    def layer_step(x_cur, weights):
        x_next, normed, pre_act, hidden = layer_forward(x_cur, weights[0], weights[1])
        return x_next, (x_cur, normed, pre_act, hidden)

    def back_step(d_cur, stored):
        x_in, normed, pre_act, hidden, up_mat, down_mat = stored
        d_in, grad_up, grad_down = layer_backward(d_cur, x_in, normed, pre_act, hidden, up_mat, down_mat)
        return d_in, (grad_up, grad_down)

    def micro_step(grads, batch):
        x_batch, g_batch = batch
        x_last, stored = lax.scan(layer_step, x_batch, (w_up, w_down))
        d_first, layer_grads = lax.scan(back_step, g_batch, stored + (w_up, w_down), reverse=True)
        return (grads[0] + layer_grads[0], grads[1] + layer_grads[1]), (x_last, d_first)

    zero_grads = (jnp.zeros(w_up.shape, jnp.float32), jnp.zeros(w_down.shape, jnp.float32))
    totals, outputs = lax.scan(micro_step, zero_grads, (tokens, cotangent))
    return outputs[0], outputs[1], totals[0], totals[1]
```

```python
import jax
import jax.numpy as jnp
from jax import lax
from jax.sharding import PartitionSpec as P

NORM_EPS = 1e-6
ALL_AXES = ("local", "data")
PAD = 48


def norm_f32(x_f32):
    return x_f32 * lax.rsqrt(jnp.mean(x_f32 * x_f32, axis=-1, keepdims=True) + NORM_EPS)


def gelu_f32(pre_f32):
    return jax.nn.gelu(pre_f32, approximate=True)


def solution(mesh):
    n_data = mesh.shape["data"]
    n_local = mesh.shape["local"]

    def body(tokens, cotangent, w_up, w_down):
        micro, rows, hidden = tokens.shape
        layers, up_rows, ffn = w_up.shape
        down_rows = w_down.shape[1]
        pad = PAD - down_rows
        width = n_local * PAD

        up = w_up.reshape(layers, up_rows, n_local, n_data, down_rows)
        up = jnp.pad(up, ((0, 0),) * 4 + ((0, pad),))
        up = up.transpose(3, 0, 1, 2, 4).reshape(n_data, layers, up_rows, width)
        up = lax.all_to_all(up, "data", 0, 0)
        up = up.transpose(1, 0, 2, 3).reshape(layers, n_data * up_rows, width)
        down = jnp.pad(w_down, ((0, 0), (0, pad), (0, 0)))

        def gather_weights(layer, after=None):
            u, d = up[layer], down[layer]
            if after is not None:
                u, d, _ = lax.optimization_barrier((u, d, after))
            return (lax.all_gather(u, "local", axis=0, tiled=True),
                    lax.all_gather(d, "local", axis=0, tiled=True))

        x_cur = tokens.reshape(micro * rows, hidden)
        saved = []
        for layer in range(layers):
            w1, w2 = gather_weights(layer)
            x_f32 = x_cur.astype(jnp.float32)
            normed = norm_f32(x_f32).astype(jnp.bfloat16)
            u_all = lax.all_gather(normed, "data", axis=0, tiled=True)
            pre = jnp.dot(u_all, w1, preferred_element_type=jnp.float32).astype(jnp.bfloat16)
            act = gelu_f32(pre.astype(jnp.float32)).astype(jnp.bfloat16)
            part = jnp.dot(act, w2, preferred_element_type=jnp.float32)
            y = lax.psum_scatter(part, "data", scatter_dimension=0, tiled=True)
            saved.append((x_cur, u_all, pre, act))
            x_cur = (x_f32 + y).astype(jnp.bfloat16)
        x_final = x_cur

        d_cur = cotangent.reshape(micro * rows, hidden)
        grads_up = [None] * layers
        grads_down = [None] * layers
        after = part
        for layer in reversed(range(layers)):
            x_in, u_all, pre, act = saved[layer]
            w1, w2 = gather_weights(layer, after)
            c_all = lax.all_gather(d_cur, "data", axis=0, tiled=True)
            e = jnp.einsum("tm,fm->tf", c_all, w2, preferred_element_type=jnp.float32)
            z = jax.vjp(gelu_f32, pre.astype(jnp.float32))[1](e)[0].astype(jnp.bfloat16)
            part = jnp.einsum("tf,mf->tm", z, w1, preferred_element_type=jnp.float32)
            v = lax.psum_scatter(part, "data", scatter_dimension=0, tiled=True)
            d_w1 = jnp.einsum("tm,tf->mf", u_all, z, preferred_element_type=jnp.float32)
            d_w2 = jnp.einsum("tf,tm->fm", act, c_all, preferred_element_type=jnp.float32)
            grads_up[layer] = lax.psum_scatter(d_w1, "local", scatter_dimension=0, tiled=True)
            grads_down[layer] = lax.psum_scatter(d_w2, "local", scatter_dimension=0, tiled=True)[:down_rows]
            norm_pull = jax.vjp(norm_f32, x_in.astype(jnp.float32))[1]
            d_cur = (d_cur.astype(jnp.float32) + norm_pull(v)[0]).astype(jnp.bfloat16)
            after = z
        g_up = jnp.stack(grads_up).reshape(layers, n_data, up_rows, width).transpose(1, 0, 2, 3)
        g_up = lax.all_to_all(g_up, "data", 0, 0)
        g_up = g_up.reshape(n_data, layers, up_rows, n_local, PAD)[..., :down_rows]
        g_up = g_up.transpose(1, 2, 3, 0, 4).reshape(layers, up_rows, ffn)
        shape = (micro, rows, hidden)
        return x_final.reshape(shape), d_cur.reshape(shape), g_up, jnp.stack(grads_down)

    spec = P(None, ALL_AXES, None)
    return jax.shard_map(body, mesh=mesh, in_specs=(spec,) * 4, out_specs=(spec,) * 4, check_vma=False)
```

```python
import functools

import jax
import jax.numpy as jnp
from jax import lax
from jax.experimental import pallas as pl
from jax.experimental.pallas import tpu as pltpu
from jax.sharding import PartitionSpec as P

NORM_EPS = 1e-6
ALL_AXES = ("local", "data")
PAD = 48
RING = 4
CORES = 2
MESH = pl.DeviceIdType.MESH


def norm_f32(x_f32):
    return x_f32 * lax.rsqrt(jnp.mean(x_f32 * x_f32, axis=-1, keepdims=True) + NORM_EPS)


def gelu_f32(pre_f32):
    return jax.nn.gelu(pre_f32, approximate=True)


class Place:
    def __init__(self):
        local, data = lax.axis_index("local"), lax.axis_index("data")
        self.z, self.y = local // RING, local % RING
        self.x, self.core = data // CORES, data % CORES

    def dev(self, z=None, y=None, x=None, core=None):
        z, y = self.z if z is None else z, self.y if y is None else y
        x, core = self.x if x is None else x, self.core if core is None else core
        return (z * RING + y, x * CORES + core)

    def along(self, axis):
        me = getattr(self, axis)
        right, left = lax.rem(me + 1, RING), lax.rem(me + RING - 1, RING)
        return me, self.dev(**{axis: right}), self.dev(**{axis: left})

    def sibling(self):
        return self.dev(core=1 - self.core)


def greet(devices):
    barrier = pltpu.get_barrier_semaphore()
    for device in devices:
        pl.semaphore_signal(barrier, inc=1, device_id=device, device_id_type=MESH)
    pl.semaphore_wait(barrier, len(devices))


class Sender:
    def __init__(self, send_sems, recv_sems):
        self.send_sems, self.recv_sems, self.started = send_sems, recv_sems, []

    def copy(self, slot, src, dst, device):
        c = pltpu.make_async_remote_copy(src_ref=src, dst_ref=dst, send_sem=self.send_sems.at[slot],
                                         recv_sem=self.recv_sems.at[slot], device_id=device, device_id_type=MESH)
        return c

    def start(self, slot, src, dst, device):
        c = self.copy(slot, src, dst, device)
        c.start()
        self.started.append(c)

    def arrived(self, slot, dst, device):
        self.copy(slot, dst, dst, device).wait_recv()

    def drain(self):
        for c in self.started:
            c.wait_send()


class RingGather:
    def __init__(self, sender, base, ring, own, block):
        self.s, self.base, self.own, self.block = sender, base, own, block
        self.me, self.right, self.left = ring
        self.prev, self.next = lax.rem(self.me + 3, RING), lax.rem(self.me + 1, RING)
        self.far = lax.rem(self.me + 2, RING)

    def start(self):
        for h in (0, 1):
            self.s.start(self.base + h, self.own(h), self.block(self.me, h), self.right)
            self.s.start(self.base + 3 - h, self.own(1 - h), self.block(self.me, 1 - h), self.left)

    def relay(self):
        self.s.arrived(self.base, self.block(self.prev, 0), self.left)
        self.s.start(self.base + 4, self.block(self.prev, 0), self.block(self.prev, 0), self.right)
        self.s.arrived(self.base + 3, self.block(self.next, 1), self.right)
        self.s.start(self.base + 5, self.block(self.next, 1), self.block(self.next, 1), self.left)

    def near(self):
        self.s.arrived(self.base + 1, self.block(self.prev, 1), self.left)
        self.s.arrived(self.base + 2, self.block(self.next, 0), self.right)

    def finish(self):
        self.s.arrived(self.base + 4, self.block(self.far, 0), self.left)
        self.s.arrived(self.base + 5, self.block(self.far, 1), self.right)


def gather_kernel(x_ref, up_ref, down_ref, xs_ref, w1_ref, w2_ref, send_sems, recv_sems, local_sems):
    p = Place()
    ring_x, ring_y, ring_z = p.along("x"), p.along("y"), p.along("z")
    sib, c, o = p.sibling(), p.core, 1 - p.core
    keep = [pltpu.make_async_copy(x_ref, xs_ref.at[p.x, c], local_sems.at[0]),
            pltpu.make_async_copy(up_ref, w1_ref.at[p.z, p.y], local_sems.at[1]),
            pltpu.make_async_copy(down_ref, w2_ref.at[p.z, p.y], local_sems.at[2])]
    for copy in keep:
        copy.start()
    greet([ring_x[1], ring_x[2], ring_y[1], ring_y[2], ring_z[1], ring_z[2], sib])
    s = Sender(send_sems, recv_sems)
    rows, cols = up_ref.shape[0] // 2, down_ref.shape[1] // 2
    gx = RingGather(s, 0, ring_x, lambda h: x_ref.at[h], lambda i, h: xs_ref.at[i, c, h])
    up1 = RingGather(s, 6, ring_y, lambda h: up_ref.at[pl.ds(h * rows, rows)],
                     lambda i, h: w1_ref.at[p.z, i, pl.ds(h * rows, rows)])
    down1 = RingGather(s, 12, ring_z, lambda h: down_ref.at[:, pl.ds(h * cols, cols)],
                       lambda i, h: w2_ref.at[i, p.y, :, pl.ds(h * cols, cols)])
    up2 = RingGather(s, 18, ring_z, lambda h: w1_ref.at[p.z, pl.ds(2 * h, 2)],
                     lambda i, h: w1_ref.at[i, pl.ds(2 * h, 2)])
    down2 = RingGather(s, 24, ring_y, lambda h: w2_ref.at[pl.ds(2 * h, 2), p.y],
                       lambda i, h: w2_ref.at[pl.ds(2 * h, 2), i])

    def to_sibling(k, i, h, src=None):
        s.start(30 + k, xs_ref.at[i, c, h] if src is None else src, xs_ref.at[i, c, h], sib)

    up1.start()
    down1.start()
    gx.start()
    for h in (0, 1):
        to_sibling(h, p.x, h, x_ref.at[h])
    up1.relay()
    down1.relay()
    up1.near()
    down1.near()
    up1.finish()
    down1.finish()
    for copy in keep:
        copy.wait()
    up2.start()
    down2.start()
    gx.relay()
    to_sibling(2, gx.prev, 0)
    to_sibling(3, gx.next, 1)
    up2.relay()
    down2.relay()
    gx.near()
    to_sibling(4, gx.prev, 1)
    to_sibling(5, gx.next, 0)
    up2.near()
    down2.near()
    up2.finish()
    down2.finish()
    gx.finish()
    to_sibling(6, gx.far, 0)
    to_sibling(7, gx.far, 1)
    for k, (i, h) in enumerate(((p.x, 0), (p.x, 1), (gx.prev, 0), (gx.next, 1), (gx.prev, 1), (gx.next, 0), (gx.far, 0), (gx.far, 1))):
        s.arrived(30 + k, xs_ref.at[i, o, h], sib)
    s.drain()


def gather(x, up, down):
    vmem, anywhere = pl.BlockSpec(memory_space=pltpu.VMEM), pl.BlockSpec(memory_space=pl.ANY)
    return pl.pallas_call(
        gather_kernel,
        out_shape=[jax.ShapeDtypeStruct((RING, CORES) + x.shape, x.dtype),
                   jax.ShapeDtypeStruct((RING, RING) + up.shape, up.dtype),
                   jax.ShapeDtypeStruct((RING, RING) + down.shape, down.dtype)],
        in_specs=[vmem] * 3,
        out_specs=[anywhere] * 3,
        scratch_shapes=[pltpu.SemaphoreType.DMA((38,)), pltpu.SemaphoreType.DMA((38,)), pltpu.SemaphoreType.DMA((3,))],
        compiler_params=pltpu.CompilerParams(collective_id=0, has_side_effects=True),
        cost_estimate=pl.CostEstimate(flops=0, bytes_accessed=120_000_000, transcendentals=0),
        name="gather",
    )(x, up, down)


def add_into(dst, *terms):
    rows = dst.shape[0]

    @pl.loop(0, rows // 8)
    def _(i):
        at = pl.ds(pl.multiple_of(i * 8, 8), 8)
        total = dst[at, :]
        for term in terms:
            total = total + term[at, :]
        dst[at, :] = total


def scatter_kernel(transposed, h_ref, w_ref, y_ref, to_sib, from_sib, acc, relayed, arriving, send_sems, recv_sems):
    p = Place()
    me, right, left = p.along("x")
    sib, c, o = p.sibling(), p.core, 1 - p.core
    greet([right, left, sib])
    s = Sender(send_sems, recv_sems)
    hidden = y_ref.shape[1]
    rows = y_ref.shape[0] // 2
    step = 512
    first, second = pl.ds(0, rows), pl.ds(rows, rows)

    def product(dx, core, dst):
        block = lax.rem(me + dx, RING)

        @pl.loop(0, hidden // step)
        def _(n):
            at = pl.ds(pl.multiple_of(n * step, step), step)
            if transposed:
                dst[:, at] = lax.dot_general(h_ref[block, core], w_ref[at, :], (((1,), (1,)), ((), ())),
                                             preferred_element_type=jnp.float32)
            else:
                dst[:, at] = jnp.dot(h_ref[block, core], w_ref[:, at], preferred_element_type=jnp.float32)

    def both(k, dx, dst):
        product(dx, o, to_sib.at[k])
        s.start(k, to_sib.at[k], from_sib.at[k], sib)
        product(dx, c, dst)

    def joined(k, dst):
        s.arrived(k, from_sib.at[k], sib)
        add_into(dst, from_sib.at[k])

    both(0, 2, acc.at[0])
    both(1, 1, acc.at[1])
    joined(0, acc.at[0])
    s.start(4, acc.at[0, first], relayed.at[0], right)
    s.start(5, acc.at[0, second], relayed.at[1], left)
    both(2, 3, acc.at[2])
    joined(1, acc.at[1])
    s.start(6, acc.at[1, second], arriving.at[0, second], right)
    both(3, 0, y_ref)
    joined(2, acc.at[2])
    s.start(7, acc.at[2, first], arriving.at[1, first], left)
    joined(3, y_ref)
    s.arrived(4, relayed.at[0], left)
    add_into(acc.at[1, first], relayed.at[0])
    s.start(8, acc.at[1, first], arriving.at[0, first], right)
    s.arrived(5, relayed.at[1], right)
    add_into(acc.at[2, second], relayed.at[1])
    s.start(9, acc.at[2, second], arriving.at[1, second], left)
    s.arrived(6, arriving.at[0, second], left)
    s.arrived(7, arriving.at[1, first], right)
    s.arrived(8, arriving.at[0, first], left)
    s.arrived(9, arriving.at[1, second], right)
    add_into(y_ref, arriving.at[0], arriving.at[1])
    s.drain()


def scatter(h, w, transposed):
    rows, width = h.shape[2:]
    hidden = w.shape[0] if transposed else w.shape[1]
    vmem = pl.BlockSpec(memory_space=pltpu.VMEM)
    f32 = jnp.float32
    return pl.pallas_call(
        functools.partial(scatter_kernel, transposed),
        out_shape=jax.ShapeDtypeStruct((rows, hidden), f32),
        in_specs=[vmem] * 2,
        out_specs=vmem,
        scratch_shapes=[pltpu.VMEM((RING, rows, hidden), f32), pltpu.VMEM((RING, rows, hidden), f32),
                        pltpu.VMEM((3, rows, hidden), f32), pltpu.VMEM((2, rows // 2, hidden), f32),
                        pltpu.VMEM((2, rows, hidden), f32),
                        pltpu.SemaphoreType.DMA((10,)), pltpu.SemaphoreType.DMA((10,))],
        compiler_params=pltpu.CompilerParams(collective_id=2 if transposed else 1, has_side_effects=True,
                                             vmem_limit_bytes=48 * 1024 * 1024),
        cost_estimate=pl.CostEstimate(flops=0, bytes_accessed=240_000_000, transcendentals=0),
        name="scatter_t" if transposed else "scatter",
    )(h, w)


def solution(mesh):
    n_data = mesh.shape["data"]
    n_local = mesh.shape["local"]

    def body(tokens, cotangent, w_up, w_down):
        micro, rows, hidden = tokens.shape
        layers, up_rows, ffn = w_up.shape
        down_rows = w_down.shape[1]
        pad = PAD - down_rows
        width = n_local * PAD
        own = micro * rows
        count = n_data * own

        up = w_up.reshape(layers, up_rows, n_local, n_data, down_rows)
        up = jnp.pad(up, ((0, 0),) * 4 + ((0, pad),))
        up = up.transpose(3, 0, 1, 2, 4).reshape(n_data, layers, up_rows, width)
        up = lax.all_to_all(up, "data", 0, 0)
        up = up.transpose(1, 0, 2, 3).reshape(layers, n_data * up_rows, width)
        down = jnp.pad(w_down, ((0, 0), (0, pad), (0, 0)))

        def gathered(x, layer):
            xs, w1, w2 = gather(x.reshape(micro, rows, hidden), up[layer], down[layer])
            return xs.reshape(count, hidden), w1.reshape(hidden, width), w2.reshape(width, hidden)

        def scattered(h, w, transposed):
            return scatter(h.reshape(RING, CORES, own, width), w, transposed)

        x_cur = tokens.reshape(own, hidden)
        saved = []
        for layer in range(layers):
            x_f32 = x_cur.astype(jnp.float32)
            u_all, w1, w2 = gathered(norm_f32(x_f32).astype(jnp.bfloat16), layer)
            pre = jnp.dot(u_all, w1, preferred_element_type=jnp.float32).astype(jnp.bfloat16)
            act = gelu_f32(pre.astype(jnp.float32)).astype(jnp.bfloat16)
            y = scattered(act, w2, False)
            saved.append((x_cur, u_all, pre, act))
            x_cur = (x_f32 + y).astype(jnp.bfloat16)
        x_final = x_cur

        d_cur = cotangent.reshape(own, hidden)
        d_cur, x_final = lax.optimization_barrier((d_cur, x_final))
        grads_up = [None] * layers
        grads_down = [None] * layers
        for layer in reversed(range(layers)):
            x_in, u_all, pre, act = saved[layer]
            c_all, w1, w2 = gathered(d_cur, layer)
            e = jnp.einsum("tm,fm->tf", c_all, w2, preferred_element_type=jnp.float32)
            z = jax.vjp(gelu_f32, pre.astype(jnp.float32))[1](e)[0].astype(jnp.bfloat16)
            d_w2 = jnp.einsum("tf,tm->fm", act, c_all, preferred_element_type=jnp.float32)
            d_w1 = jnp.einsum("tm,tf->mf", u_all, z, preferred_element_type=jnp.float32)
            v = scattered(z, w1, True)
            grads_up[layer] = lax.psum_scatter(d_w1, "local", scatter_dimension=0, tiled=True)
            grads_down[layer] = lax.psum_scatter(d_w2, "local", scatter_dimension=0, tiled=True)[:down_rows]
            norm_pull = jax.vjp(norm_f32, x_in.astype(jnp.float32))[1]
            d_cur = (d_cur.astype(jnp.float32) + norm_pull(v)[0]).astype(jnp.bfloat16)
        g_up = jnp.stack(grads_up).reshape(layers, n_data, up_rows, width).transpose(1, 0, 2, 3)
        g_up = lax.all_to_all(g_up, "data", 0, 0)
        g_up = g_up.reshape(n_data, layers, up_rows, n_local, PAD)[..., :down_rows]
        g_up = g_up.transpose(1, 2, 3, 0, 4).reshape(layers, up_rows, ffn)
        shape = (micro, rows, hidden)
        return x_final.reshape(shape), d_cur.reshape(shape), g_up, jnp.stack(grads_down)

    spec = P(None, ALL_AXES, None)
    return jax.shard_map(body, mesh=mesh, in_specs=(spec,) * 4, out_specs=(spec,) * 4, check_vma=False)
```

```python
import functools

import jax
import jax.numpy as jnp
from jax import lax
from jax.experimental import pallas as pl
from jax.experimental.pallas import tpu as pltpu
from jax.sharding import PartitionSpec as P

NORM_EPS = 1e-6
ALL_AXES = ("local", "data")
PAD = 48
RING = 4
CORES = 2
MESH = pl.DeviceIdType.MESH


def norm_f32(x_f32):
    return x_f32 * lax.rsqrt(jnp.mean(x_f32 * x_f32, axis=-1, keepdims=True) + NORM_EPS)


def gelu_f32(pre_f32):
    return jax.nn.gelu(pre_f32, approximate=True)


class Place:
    def __init__(self):
        local, data = lax.axis_index("local"), lax.axis_index("data")
        self.z, self.y = local // RING, local % RING
        self.x, self.core = data // CORES, data % CORES

    def dev(self, z=None, y=None, x=None, core=None):
        z, y = self.z if z is None else z, self.y if y is None else y
        x, core = self.x if x is None else x, self.core if core is None else core
        return (z * RING + y, x * CORES + core)

    def along(self, axis):
        me = getattr(self, axis)
        right, left = lax.rem(me + 1, RING), lax.rem(me + RING - 1, RING)
        return me, self.dev(**{axis: right}), self.dev(**{axis: left})

    def sibling(self):
        return self.dev(core=1 - self.core)


def greet(devices):
    barrier = pltpu.get_barrier_semaphore()
    for device in devices:
        pl.semaphore_signal(barrier, inc=1, device_id=device, device_id_type=MESH)
    pl.semaphore_wait(barrier, len(devices))


class Sender:
    def __init__(self, send_sems, recv_sems):
        self.send_sems, self.recv_sems, self.started = send_sems, recv_sems, []

    def copy(self, slot, src, dst, device):
        c = pltpu.make_async_remote_copy(src_ref=src, dst_ref=dst, send_sem=self.send_sems.at[slot],
                                         recv_sem=self.recv_sems.at[slot], device_id=device, device_id_type=MESH)
        return c

    def start(self, slot, src, dst, device):
        c = self.copy(slot, src, dst, device)
        c.start()
        self.started.append(c)

    def arrived(self, slot, dst, device):
        self.copy(slot, dst, dst, device).wait_recv()

    def drain(self):
        for c in self.started:
            c.wait_send()


class RingGather:
    def __init__(self, sender, base, ring, own, block):
        self.s, self.base, self.own, self.block = sender, base, own, block
        self.me, self.right, self.left = ring
        self.prev, self.next = lax.rem(self.me + 3, RING), lax.rem(self.me + 1, RING)
        self.far = lax.rem(self.me + 2, RING)

    def start(self):
        for h in (0, 1):
            self.s.start(self.base + h, self.own(h), self.block(self.me, h), self.right)
            self.s.start(self.base + 3 - h, self.own(1 - h), self.block(self.me, 1 - h), self.left)

    def relay(self):
        self.s.arrived(self.base, self.block(self.prev, 0), self.left)
        self.s.start(self.base + 4, self.block(self.prev, 0), self.block(self.prev, 0), self.right)
        self.s.arrived(self.base + 3, self.block(self.next, 1), self.right)
        self.s.start(self.base + 5, self.block(self.next, 1), self.block(self.next, 1), self.left)

    def near(self):
        self.s.arrived(self.base + 1, self.block(self.prev, 1), self.left)
        self.s.arrived(self.base + 2, self.block(self.next, 0), self.right)

    def finish(self):
        self.s.arrived(self.base + 4, self.block(self.far, 0), self.left)
        self.s.arrived(self.base + 5, self.block(self.far, 1), self.right)


def gather_kernel(x_ref, up_ref, down_ref, xs_ref, w1_ref, w2_ref, send_sems, recv_sems, local_sems):
    p = Place()
    ring_x, ring_y, ring_z = p.along("x"), p.along("y"), p.along("z")
    sib, c, o = p.sibling(), p.core, 1 - p.core
    keep = [pltpu.make_async_copy(x_ref, xs_ref.at[p.x, c], local_sems.at[0]),
            pltpu.make_async_copy(up_ref, w1_ref.at[p.z, p.y], local_sems.at[1]),
            pltpu.make_async_copy(down_ref, w2_ref.at[p.z, p.y], local_sems.at[2])]
    for copy in keep:
        copy.start()
    greet([ring_x[1], ring_x[2], ring_y[1], ring_y[2], ring_z[1], ring_z[2], sib])
    s = Sender(send_sems, recv_sems)
    rows, cols = up_ref.shape[0] // 2, down_ref.shape[1] // 2
    gx = RingGather(s, 0, ring_x, lambda h: x_ref.at[h], lambda i, h: xs_ref.at[i, c, h])
    up1 = RingGather(s, 6, ring_y, lambda h: up_ref.at[pl.ds(h * rows, rows)],
                     lambda i, h: w1_ref.at[p.z, i, pl.ds(h * rows, rows)])
    down1 = RingGather(s, 12, ring_z, lambda h: down_ref.at[:, pl.ds(h * cols, cols)],
                       lambda i, h: w2_ref.at[i, p.y, :, pl.ds(h * cols, cols)])
    up2 = RingGather(s, 18, ring_z, lambda h: w1_ref.at[p.z, pl.ds(2 * h, 2)],
                     lambda i, h: w1_ref.at[i, pl.ds(2 * h, 2)])
    down2 = RingGather(s, 24, ring_y, lambda h: w2_ref.at[pl.ds(2 * h, 2), p.y],
                       lambda i, h: w2_ref.at[pl.ds(2 * h, 2), i])

    def to_sibling(k, i, h, src=None):
        s.start(30 + k, xs_ref.at[i, c, h] if src is None else src, xs_ref.at[i, c, h], sib)

    up1.start()
    down1.start()
    gx.start()
    for h in (0, 1):
        to_sibling(h, p.x, h, x_ref.at[h])
    up1.relay()
    down1.relay()
    up1.near()
    down1.near()
    up1.finish()
    down1.finish()
    for copy in keep:
        copy.wait()
    up2.start()
    down2.start()
    gx.relay()
    to_sibling(2, gx.prev, 0)
    to_sibling(3, gx.next, 1)
    up2.relay()
    down2.relay()
    gx.near()
    to_sibling(4, gx.prev, 1)
    to_sibling(5, gx.next, 0)
    up2.near()
    down2.near()
    up2.finish()
    down2.finish()
    gx.finish()
    to_sibling(6, gx.far, 0)
    to_sibling(7, gx.far, 1)
    for k, (i, h) in enumerate(((p.x, 0), (p.x, 1), (gx.prev, 0), (gx.next, 1), (gx.prev, 1), (gx.next, 0), (gx.far, 0), (gx.far, 1))):
        s.arrived(30 + k, xs_ref.at[i, o, h], sib)
    s.drain()


def gather(x, up, down):
    vmem, anywhere = pl.BlockSpec(memory_space=pltpu.VMEM), pl.BlockSpec(memory_space=pl.ANY)
    return pl.pallas_call(
        gather_kernel,
        out_shape=[jax.ShapeDtypeStruct((RING, CORES) + x.shape, x.dtype),
                   jax.ShapeDtypeStruct((RING, RING) + up.shape, up.dtype),
                   jax.ShapeDtypeStruct((RING, RING) + down.shape, down.dtype)],
        in_specs=[vmem] * 3,
        out_specs=[anywhere] * 3,
        scratch_shapes=[pltpu.SemaphoreType.DMA((38,)), pltpu.SemaphoreType.DMA((38,)), pltpu.SemaphoreType.DMA((3,))],
        compiler_params=pltpu.CompilerParams(collective_id=0, has_side_effects=True),
        cost_estimate=pl.CostEstimate(flops=0, bytes_accessed=120_000_000, transcendentals=0),
        name="gather",
    )(x, up, down)


def add_into(dst, *terms):
    if len(dst.shape) > 2:
        for i in range(dst.shape[0]):
            add_into(dst.at[i], *(term.at[i] for term in terms))
        return

    @pl.loop(0, dst.shape[0] // 8)
    def _(i):
        at = pl.ds(pl.multiple_of(i * 8, 8), 8)
        total = dst[at, :]
        for term in terms:
            total = total + term[at, :]
        dst[at, :] = total


class RingScatter:
    def __init__(self, sender, base, ring, block, relayed, arriving):
        self.s, self.base, self.block, self.relayed, self.arriving = sender, base, block, relayed, arriving
        self.me, self.right, self.left = ring
        self.prev, self.next = lax.rem(self.me + 3, RING), lax.rem(self.me + 1, RING)
        self.far = lax.rem(self.me + 2, RING)

    def start(self):
        self.s.start(self.base, self.block(self.far, 0), self.relayed(0), self.right)
        self.s.start(self.base + 1, self.block(self.far, 1), self.relayed(1), self.left)
        self.s.start(self.base + 2, self.block(self.next, 1), self.arriving(0, 1), self.right)
        self.s.start(self.base + 3, self.block(self.prev, 0), self.arriving(1, 0), self.left)

    def relay(self, to_next, to_prev):
        self.s.arrived(self.base, self.relayed(0), self.left)
        add_into(self.relayed(0), to_next)
        self.s.start(self.base + 4, self.relayed(0), self.arriving(0, 0), self.right)
        self.s.arrived(self.base + 1, self.relayed(1), self.right)
        add_into(self.relayed(1), to_prev)
        self.s.start(self.base + 5, self.relayed(1), self.arriving(1, 1), self.left)

    def finish(self):
        self.s.arrived(self.base + 2, self.arriving(0, 1), self.left)
        self.s.arrived(self.base + 3, self.arriving(1, 0), self.right)
        self.s.arrived(self.base + 4, self.arriving(0, 0), self.left)
        self.s.arrived(self.base + 5, self.arriving(1, 1), self.right)


class GradScatter:
    SLOTS = 24

    def __init__(self, p, sender, base, up, down, bufs, sems):
        self.p, self.sems, self.up, self.down = p, sems, up, down
        (self.u_rel, self.u_arr, self.u_loc, self.u_own, self.u_rel2, self.u_arr2,
         self.d_rel, self.d_arr, self.d_loc, self.d_own, self.d_rel2, self.d_arr2) = bufs
        ring_y, ring_z = p.along("y"), p.along("z")
        half = lambda h: pl.ds(2 * h, 2)
        u_rows, d_rows = up.shape[2] // 2, down.shape[2] // 2
        u_part, d_part = (lambda h: pl.ds(h * u_rows, u_rows)), (lambda h: pl.ds(h * d_rows, d_rows))
        self.up1 = RingScatter(sender, base, ring_y, lambda i, h: up.at[half(h), i], lambda h: self.u_rel.at[h],
                               lambda side, h: self.u_arr.at[side, half(h)])
        self.down1 = RingScatter(sender, base + 6, ring_z, lambda i, h: down.at[i, half(h)], lambda h: self.d_rel.at[h],
                                 lambda side, h: self.d_arr.at[side, half(h)])
        self.up2 = RingScatter(sender, base + 12, ring_z, lambda i, h: self.u_own.at[i, u_part(h)], lambda h: self.u_rel2.at[h],
                               lambda side, h: self.u_arr2.at[side, u_part(h)])
        self.down2 = RingScatter(sender, base + 18, ring_y, lambda i, h: self.d_own.at[i, d_part(h)], lambda h: self.d_rel2.at[h],
                                 lambda side, h: self.d_arr2.at[side, d_part(h)])
        self.u_part, self.d_part = u_part, d_part
        u, d = self.up1, self.down1
        pairs = [(up.at[half(0), u.next], self.u_loc.at[0]), (up.at[half(1), u.prev], self.u_loc.at[1]),
                 (up.at[:, u.me], self.u_own), (down.at[d.next, half(0)], self.d_loc.at[0]),
                 (down.at[d.prev, half(1)], self.d_loc.at[1]), (down.at[d.me], self.d_own)]
        self.loads = [pltpu.make_async_copy(src, dst, sems.at[k]) for k, (src, dst) in enumerate(pairs)]

    def load(self):
        for copy in self.loads:
            copy.start()

    def start(self):
        self.up1.start()
        self.down1.start()

    def relay(self):
        for copy in self.loads:
            copy.wait()
        self.up1.relay(self.u_loc.at[0], self.u_loc.at[1])
        self.down1.relay(self.d_loc.at[0], self.d_loc.at[1])

    def second(self):
        self.up1.finish()
        add_into(self.u_own, self.u_arr.at[0], self.u_arr.at[1])
        self.up2.start()
        self.down1.finish()
        add_into(self.d_own, self.d_arr.at[0], self.d_arr.at[1])
        self.down2.start()
        u, d = self.up2, self.down2
        u.relay(self.u_own.at[u.next, self.u_part(0)], self.u_own.at[u.prev, self.u_part(1)])
        d.relay(self.d_own.at[d.next, self.d_part(0)], self.d_own.at[d.prev, self.d_part(1)])

    def finish(self, up_out, down_out):
        self.up2.finish()
        self.down2.finish()
        up_out[...] = self.u_own[self.up2.me] + self.u_arr2[0] + self.u_arr2[1]
        down_out[...] = self.d_own[self.down2.me] + self.d_arr2[0] + self.d_arr2[1]

    @staticmethod
    def buffers(up, down):
        f32 = jnp.float32
        out = []
        for rows, cols in (up.shape[2:], down.shape[2:]):
            out += [(2, 2, rows, cols), (2, RING, rows, cols), (2, 2, rows, cols), (RING, rows, cols),
                    (2, rows // 2, cols), (2, rows, cols)]
        return [pltpu.VMEM(shape, f32) for shape in out]


def scatter_kernel(h_ref, w_ref, *refs):
    backward = len(refs) > 8
    p = Place()
    me, right, left = p.along("x")
    sib, c, o = p.sibling(), p.core, 1 - p.core
    if backward:
        (g_up, g_down, y_ref, up_out, down_out, to_sib, from_sib, acc, relayed, arriving, send_sems, recv_sems,
         up_sum, local_sems, *bufs) = refs
        ring_y, ring_z = p.along("y"), p.along("z")
        others = [p.dev(x=lax.rem(me + dx, RING), core=lax.rem(c + dc, CORES)) for dx in range(RING) for dc in range(CORES)][1:]
        greet(others + [ring_y[1], ring_y[2], ring_z[1], ring_z[2]])
        s = Sender(send_sems, recv_sems)
        grads = GradScatter(p, s, 10, g_up, g_down, bufs, local_sems)
        grads.start()
        grads.load()
    else:
        y_ref, to_sib, from_sib, acc, relayed, arriving, send_sems, recv_sems = refs
        greet([right, left, sib])
        s = Sender(send_sems, recv_sems)
    hidden = y_ref.shape[1]
    rows = y_ref.shape[0] // 2
    step = 512
    first, second = pl.ds(0, rows), pl.ds(rows, rows)

    def product(dx, core, dst):
        block = lax.rem(me + dx, RING)

        @pl.loop(0, hidden // step)
        def _(n):
            at = pl.ds(pl.multiple_of(n * step, step), step)
            if backward:
                dst[:, at] = lax.dot_general(h_ref[block, core], w_ref[at, :], (((1,), (1,)), ((), ())),
                                             preferred_element_type=jnp.float32)
            else:
                dst[:, at] = jnp.dot(h_ref[block, core], w_ref[:, at], preferred_element_type=jnp.float32)

    def both(k, dx, dst):
        product(dx, o, to_sib.at[k])
        s.start(k, to_sib.at[k], from_sib.at[k], sib)
        product(dx, c, dst)

    def joined(k, dst):
        s.arrived(k, from_sib.at[k], sib)
        add_into(dst, from_sib.at[k])

    both(0, 2, acc.at[0])
    joined(0, acc.at[0])
    s.start(4, acc.at[0, first], relayed.at[0], right)
    s.start(5, acc.at[0, second], relayed.at[1], left)
    both(1, 1, acc.at[1])
    both(2, 3, acc.at[2])
    joined(1, acc.at[1])
    s.start(6, acc.at[1, second], arriving.at[0, second], right)
    joined(2, acc.at[2])
    s.start(7, acc.at[2, first], arriving.at[1, first], left)
    both(3, 0, y_ref)
    joined(3, y_ref)
    if backward:
        grads.relay()
    s.arrived(4, relayed.at[0], left)
    add_into(acc.at[1, first], relayed.at[0])
    s.start(8, acc.at[1, first], arriving.at[0, first], right)
    s.arrived(5, relayed.at[1], right)
    add_into(acc.at[2, second], relayed.at[1])
    s.start(9, acc.at[2, second], arriving.at[1, second], left)
    if backward:
        grads.second()
        grads.finish(up_sum, down_out)
        mine = me * CORES + c
        piece = up_out.shape[1]
        keep = pltpu.make_async_copy(up_sum.at[pl.ds(pl.multiple_of(mine * piece, piece), piece)], up_out.at[mine], local_sems.at[6])
        keep.start()
        turns = [(lax.rem(me + dx, RING), lax.rem(c + dc, CORES)) for dx in range(RING) for dc in range(CORES)][1:]
        for k, (x, core) in enumerate(turns):
            to = x * CORES + core
            s.start(34 + k, up_sum.at[pl.ds(pl.multiple_of(to * piece, piece), piece)], up_out.at[mine], p.dev(x=x, core=core))
    s.arrived(6, arriving.at[0, second], left)
    s.arrived(7, arriving.at[1, first], right)
    s.arrived(8, arriving.at[0, first], left)
    s.arrived(9, arriving.at[1, second], right)
    add_into(y_ref, arriving.at[0], arriving.at[1])
    if backward:
        for k in range(len(turns)):
            dx, dc = divmod(k + 1, CORES)
            x, core = lax.rem(me + RING - dx, RING), lax.rem(c + dc, CORES)
            s.arrived(34 + k, up_out.at[x * CORES + core], p.dev(x=x, core=core))
        keep.wait()
    s.drain()


def scatter(h, w, grads=None):
    rows, width = h.shape[2:]
    hidden = w.shape[1] if grads is None else w.shape[0]
    vmem, anywhere = pl.BlockSpec(memory_space=pltpu.VMEM), pl.BlockSpec(memory_space=pl.ANY)
    f32 = jnp.float32
    outs = [jax.ShapeDtypeStruct((rows, hidden), f32)]
    slots = 10
    extra = []
    if grads is not None:
        up_rows, down_rows = grads[0].shape[2], grads[1].shape[2]
        n_data = RING * CORES
        outs += [jax.ShapeDtypeStruct((n_data, up_rows // n_data, width), f32), jax.ShapeDtypeStruct((down_rows, hidden), f32)]
        slots = 10 + GradScatter.SLOTS + n_data - 1
        extra = [pltpu.VMEM((up_rows, width), f32), pltpu.SemaphoreType.DMA((7,))] + GradScatter.buffers(*grads)
    return pl.pallas_call(
        scatter_kernel,
        out_shape=outs,
        in_specs=[vmem] * 2 + [anywhere] * (0 if grads is None else 2),
        out_specs=[vmem] * len(outs),
        scratch_shapes=[pltpu.VMEM((RING, rows, hidden), f32), pltpu.VMEM((RING, rows, hidden), f32),
                        pltpu.VMEM((3, rows, hidden), f32), pltpu.VMEM((2, rows // 2, hidden), f32),
                        pltpu.VMEM((2, rows, hidden), f32),
                        pltpu.SemaphoreType.DMA((slots,)), pltpu.SemaphoreType.DMA((slots,))] + extra,
        compiler_params=pltpu.CompilerParams(collective_id=1 if grads is None else 2, has_side_effects=True,
                                             vmem_limit_bytes=(44 if grads is None else 62) * 1024 * 1024),
        cost_estimate=pl.CostEstimate(flops=0, bytes_accessed=240_000_000, transcendentals=0),
        name="scatter" if grads is None else "scatter_grads",
    )(h, w, *(grads or ()))


def solution(mesh):
    n_data = mesh.shape["data"]
    n_local = mesh.shape["local"]

    def body(tokens, cotangent, w_up, w_down):
        micro, rows, hidden = tokens.shape
        layers, up_rows, ffn = w_up.shape
        down_rows = w_down.shape[1]
        pad = PAD - down_rows
        width = n_local * PAD
        own = micro * rows
        count = n_data * own

        up = w_up.reshape(layers, up_rows, n_local, n_data, down_rows)
        up = jnp.pad(up, ((0, 0),) * 4 + ((0, pad),))
        up = up.transpose(3, 0, 1, 2, 4).reshape(n_data, layers, up_rows, width)
        up = lax.all_to_all(up, "data", 0, 0)
        up = up.transpose(1, 0, 2, 3).reshape(layers, n_data * up_rows, width)
        down = jnp.pad(w_down, ((0, 0), (0, pad), (0, 0)))

        def gathered(x, layer):
            xs, w1, w2 = gather(x.reshape(micro, rows, hidden), up[layer], down[layer])
            return xs.reshape(count, hidden), w1.reshape(hidden, width), w2.reshape(width, hidden)

        def blocks(h):
            return h.reshape(RING, CORES, own, width)

        x_cur = tokens.reshape(own, hidden)
        saved = []
        for layer in range(layers):
            x_f32 = x_cur.astype(jnp.float32)
            u_all, w1, w2 = gathered(norm_f32(x_f32).astype(jnp.bfloat16), layer)
            pre = jnp.dot(u_all, w1, preferred_element_type=jnp.float32).astype(jnp.bfloat16)
            act = gelu_f32(pre.astype(jnp.float32)).astype(jnp.bfloat16)
            y, = scatter(blocks(act), w2)
            saved.append((x_cur, u_all, pre, act))
            x_cur = (x_f32 + y).astype(jnp.bfloat16)
        x_final = x_cur

        d_cur = cotangent.reshape(own, hidden)
        d_cur, x_final = lax.optimization_barrier((d_cur, x_final))
        grads_up = [None] * layers
        grads_down = [None] * layers
        for layer in reversed(range(layers)):
            x_in, u_all, pre, act = saved[layer]
            c_all, w1, w2 = gathered(d_cur, layer)
            e = jnp.einsum("tm,fm->tf", c_all, w2, preferred_element_type=jnp.float32)
            z = jax.vjp(gelu_f32, pre.astype(jnp.float32))[1](e)[0].astype(jnp.bfloat16)
            d_w2 = jnp.einsum("tf,tm->fm", act, c_all, preferred_element_type=jnp.float32)
            d_w1 = jnp.einsum("tm,tf->mf", u_all, z, preferred_element_type=jnp.float32)
            g_up, g_down = (g.reshape((RING, RING, -1) + g.shape[1:]) for g in (d_w1, d_w2))
            v, grads_up[layer], g_down = scatter(blocks(z), w1, (g_up, g_down))
            grads_down[layer] = g_down[:down_rows]
            norm_pull = jax.vjp(norm_f32, x_in.astype(jnp.float32))[1]
            d_cur = (d_cur.astype(jnp.float32) + norm_pull(v)[0]).astype(jnp.bfloat16)
        g_up = jnp.stack(grads_up, 1).reshape(n_data, layers, up_rows, n_local, PAD)[..., :down_rows]
        g_up = g_up.transpose(1, 2, 3, 0, 4).reshape(layers, up_rows, ffn)
        shape = (micro, rows, hidden)
        return x_final.reshape(shape), d_cur.reshape(shape), g_up, jnp.stack(grads_down)

    spec = P(None, ALL_AXES, None)
    return jax.shard_map(body, mesh=mesh, in_specs=(spec,) * 4, out_specs=(spec,) * 4, check_vma=False)
```

```python
import functools

import jax
import jax.numpy as jnp
from jax import lax
from jax.experimental import pallas as pl
from jax.experimental.pallas import tpu as pltpu
from jax.sharding import PartitionSpec as P

NORM_EPS = 1e-6
ALL_AXES = ("local", "data")
PAD = 48
RING = 4
CORES = 2
MESH = pl.DeviceIdType.MESH


def norm_f32(x_f32):
    return x_f32 * lax.rsqrt(jnp.mean(x_f32 * x_f32, axis=-1, keepdims=True) + NORM_EPS)


def gelu_f32(pre_f32):
    return jax.nn.gelu(pre_f32, approximate=True)


class Place:
    def __init__(self):
        local, data = lax.axis_index("local"), lax.axis_index("data")
        self.z, self.y = local // RING, local % RING
        self.x, self.core = data // CORES, data % CORES

    def dev(self, z=None, y=None, x=None, core=None):
        z, y = self.z if z is None else z, self.y if y is None else y
        x, core = self.x if x is None else x, self.core if core is None else core
        return (z * RING + y, x * CORES + core)

    def along(self, axis):
        me = getattr(self, axis)
        right, left = lax.rem(me + 1, RING), lax.rem(me + RING - 1, RING)
        return me, self.dev(**{axis: right}), self.dev(**{axis: left})

    def sibling(self):
        return self.dev(core=1 - self.core)


def greet(devices):
    barrier = pltpu.get_barrier_semaphore()
    for device in devices:
        pl.semaphore_signal(barrier, inc=1, device_id=device, device_id_type=MESH)
    pl.semaphore_wait(barrier, len(devices))


class Sender:
    def __init__(self, send_sems, recv_sems):
        self.send_sems, self.recv_sems, self.started = send_sems, recv_sems, []

    def copy(self, slot, src, dst, device):
        c = pltpu.make_async_remote_copy(src_ref=src, dst_ref=dst, send_sem=self.send_sems.at[slot],
                                         recv_sem=self.recv_sems.at[slot], device_id=device, device_id_type=MESH)
        return c

    def start(self, slot, src, dst, device):
        c = self.copy(slot, src, dst, device)
        c.start()
        self.started.append(c)

    def arrived(self, slot, dst, device):
        self.copy(slot, dst, dst, device).wait_recv()

    def drain(self):
        for c in self.started:
            c.wait_send()


class RingGather:
    def __init__(self, sender, base, ring, own, block):
        self.s, self.base, self.own, self.block = sender, base, own, block
        self.me, self.right, self.left = ring
        self.prev, self.next = lax.rem(self.me + 3, RING), lax.rem(self.me + 1, RING)
        self.far = lax.rem(self.me + 2, RING)

    def start(self):
        for h in (0, 1):
            self.s.start(self.base + h, self.own(h), self.block(self.me, h), self.right)
            self.s.start(self.base + 3 - h, self.own(1 - h), self.block(self.me, 1 - h), self.left)

    def relay(self):
        self.s.arrived(self.base, self.block(self.prev, 0), self.left)
        self.s.start(self.base + 4, self.block(self.prev, 0), self.block(self.prev, 0), self.right)
        self.s.arrived(self.base + 3, self.block(self.next, 1), self.right)
        self.s.start(self.base + 5, self.block(self.next, 1), self.block(self.next, 1), self.left)

    def near(self):
        self.s.arrived(self.base + 1, self.block(self.prev, 1), self.left)
        self.s.arrived(self.base + 2, self.block(self.next, 0), self.right)

    def finish(self):
        self.s.arrived(self.base + 4, self.block(self.far, 0), self.left)
        self.s.arrived(self.base + 5, self.block(self.far, 1), self.right)


class WeightGather:
    def __init__(self, p, sender, base, src, dst):
        ring_y, ring_z = p.along("y"), p.along("z")
        rows, cols = src.shape
        if rows >= 64:
            quarter = rows // 4
            sub = lambda part, h: (pl.ds((2 * part + h) * quarter, quarter), slice(None))
        else:
            quarter = cols // 4
            sub = lambda part, h: (slice(None), pl.ds((2 * part + h) * quarter, quarter))
        block2 = (lambda i, h: dst.at[(i, slice(None)) + sub(0, h)], lambda i, h: dst.at[(slice(None), i) + sub(1, h)])
        self.stage1 = (RingGather(sender, base, ring_y, lambda h: src.at[sub(0, h)], lambda i, h: dst.at[(p.z, i) + sub(0, h)]),
                       RingGather(sender, base + 6, ring_z, lambda h: src.at[sub(1, h)], lambda i, h: dst.at[(i, p.y) + sub(1, h)]))
        self.stage2 = (RingGather(sender, base + 12, ring_z, lambda h: block2[0](p.z, h), block2[0]),
                       RingGather(sender, base + 18, ring_y, lambda h: block2[1](p.y, h), block2[1]))

    def start(self):
        for g in self.stage1:
            g.start()

    def second(self, keep=None):
        for g in self.stage1:
            g.relay()
        for g in self.stage1:
            g.near()
            g.finish()
        if keep is not None:
            keep.wait()
        for g in self.stage2:
            g.start()

    def relay(self):
        for g in self.stage2:
            g.relay()

    def finish(self):
        for g in self.stage2:
            g.near()
            g.finish()


class Exchange:
    SLOTS = 62

    def __init__(self, x_ref, xs, first, first_dst, second, second_dst, send_sems, recv_sems, keep_sem):
        p = Place()
        ring_x, ring_y, ring_z = p.along("x"), p.along("y"), p.along("z")
        self.p, self.sib, self.xs, self.x_ref = p, p.sibling(), xs, x_ref
        c = p.core
        self.keep = pltpu.make_async_copy(second, second_dst.at[p.z, p.y], keep_sem)
        self.keep.start()
        first_dst[p.z, p.y] = first[...]
        xs[p.x, c] = x_ref[...]
        greet([ring_x[1], ring_x[2], ring_y[1], ring_y[2], ring_z[1], ring_z[2], self.sib])
        self.s = Sender(send_sems, recv_sems)
        self.gx = RingGather(self.s, 0, ring_x, lambda h: x_ref.at[h], lambda i, h: xs.at[i, c, h])
        self.first = WeightGather(p, self.s, 14, first, first_dst)
        self.second = WeightGather(p, self.s, 38, second, second_dst)

    def give(self, k, i, h, src=None):
        at = self.xs.at[i, self.p.core, h]
        self.s.start(6 + k, at if src is None else src, at, self.sib)

    def take(self, k, i, h):
        self.s.arrived(6 + k, self.xs.at[i, 1 - self.p.core, h], self.sib)

    def run(self, compute):
        gx, me = self.gx, self.p.x
        self.first.start()
        gx.start()
        for h in (0, 1):
            self.give(h, me, h, self.x_ref.at[h])
        self.second.start()
        self.first.second()
        self.second.second(self.keep)
        gx.relay()
        self.give(2, gx.prev, 0)
        self.give(3, gx.next, 1)
        self.first.relay()
        self.first.finish()
        self.second.relay()
        self.take(0, me, 0)
        self.take(1, me, 1)
        compute(me, True)
        gx.near()
        self.give(4, gx.prev, 1)
        self.give(5, gx.next, 0)
        self.take(2, gx.prev, 0)
        self.take(4, gx.prev, 1)
        compute(gx.prev, False)
        self.take(3, gx.next, 1)
        self.take(5, gx.next, 0)
        gx.finish()
        self.give(6, gx.far, 0)
        self.give(7, gx.far, 1)
        compute(gx.next, False)
        self.take(6, gx.far, 0)
        self.take(7, gx.far, 1)
        compute(gx.far, False)
        self.second.finish()
        self.s.drain()


def up_kernel(x_ref, up_ref, down_ref, u_ref, pre_ref, act_ref, w2_ref, xs, w1, wide, send_sems, recv_sems, sems):
    saves = []
    hidden, width = xs.shape[-1], w1.shape[-1]
    ex = Exchange(x_ref, xs, up_ref, w1, down_ref, w2_ref, send_sems, recv_sems, sems.at[0])

    def compute(i, _):
        save = pltpu.make_async_copy(xs.at[i], u_ref.at[i], sems.at[1 + len(saves)])
        save.start()
        saves.append(save)
        wide[...] = jnp.dot(xs[i].reshape(wide.shape[0], hidden), w1[...].reshape(hidden, width),
                            preferred_element_type=jnp.float32)

        @pl.loop(0, wide.shape[0] // 32)
        def _(r):
            at = pl.ds(pl.multiple_of(r * 32, 32), 32)
            pre = wide[at, :].astype(jnp.bfloat16)
            pre_ref[i, at, :] = pre
            act_ref[i, at, :] = gelu_f32(pre.astype(jnp.float32)).astype(jnp.bfloat16)

    ex.run(compute)
    for save in saves:
        save.wait()


def gather_up(x, up, down):
    vmem, anywhere = pl.BlockSpec(memory_space=pltpu.VMEM), pl.BlockSpec(memory_space=pl.ANY)
    micro, rows, hidden = x.shape
    block = CORES * micro * rows
    bf16, dma = jnp.bfloat16, pltpu.SemaphoreType.DMA
    return pl.pallas_call(
        up_kernel,
        out_shape=[jax.ShapeDtypeStruct((RING, CORES) + x.shape, bf16),
                   jax.ShapeDtypeStruct((RING, block, up.shape[1]), bf16),
                   jax.ShapeDtypeStruct((RING, block, up.shape[1]), bf16),
                   jax.ShapeDtypeStruct((RING, RING) + down.shape, bf16)],
        in_specs=[vmem] * 3,
        out_specs=[anywhere, vmem, vmem, anywhere],
        scratch_shapes=[pltpu.VMEM((RING, CORES) + x.shape, bf16), pltpu.VMEM((RING, RING) + up.shape, bf16),
                        pltpu.VMEM((block, up.shape[1]), jnp.float32),
                        dma((Exchange.SLOTS,)), dma((Exchange.SLOTS,)), dma((5,))],
        compiler_params=pltpu.CompilerParams(collective_id=0, has_side_effects=True, vmem_limit_bytes=40 * 1024 * 1024),
        cost_estimate=pl.CostEstimate(flops=0, bytes_accessed=120_000_000, transcendentals=0),
        name="gather_up",
    )(x, up, down)


def back_kernel(x_ref, up_ref, down_ref, u_hbm, pre_hbm, act_hbm, z_ref, w1_ref, g_up, g_down,
                xs, w2, wide, us, pres, acts, acc_up, acc_down, send_sems, recv_sems, sems):
    loads = [pltpu.make_async_copy(src, dst, sems.at[1 + k])
             for k, (src, dst) in enumerate(((pre_hbm, pres), (act_hbm, acts), (u_hbm, us)))]
    for load in loads:
        load.start()
    hidden, width = xs.shape[-1], z_ref.shape[-1]
    block = wide.shape[0]
    ex = Exchange(x_ref, xs, down_ref, w2, up_ref, w1_ref, send_sems, recv_sems, sems.at[0])
    over_rows = (((0,), (0,)), ((), ()))

    def compute(i, initial):
        if initial:
            for load in loads:
                load.wait()
        wide[...] = lax.dot_general(xs[i].reshape(block, hidden), w2[...].reshape(width, hidden), (((1,), (1,)), ((), ())),
                                    preferred_element_type=jnp.float32)

        @pl.loop(0, block // 32)
        def _(r):
            at = pl.ds(pl.multiple_of(r * 32, 32), 32)
            pull = jax.vjp(gelu_f32, pres[i, at, :].astype(jnp.float32))[1]
            z_ref[i, at, :] = pull(wide[at, :])[0].astype(jnp.bfloat16)

        step = 512

        @pl.loop(0, hidden // step)
        def _(n):
            at = pl.ds(pl.multiple_of(n * step, step), step)
            d_down = lax.dot_general(acts[i], xs.at[i, :, :, :, at][...].reshape(block, step), over_rows,
                                     preferred_element_type=jnp.float32)
            d_up = lax.dot_general(z_ref[i], us.at[i, :, :, :, at][...].reshape(block, step), over_rows,
                                   preferred_element_type=jnp.float32)
            if initial:
                acc_down[:, at] = d_down
                acc_up[:, at] = d_up
            else:
                acc_down[:, at] += d_down
                acc_up[:, at] += d_up

    ex.run(compute)
    cols, rows = g_up.shape[3], g_down.shape[2]
    copies = []
    for k in range(RING * RING):
        copies.append(pltpu.make_async_copy(acc_up.at[:, pl.ds(k * cols, cols)], g_up.at[k // RING, k % RING], sems.at[4 + k]))
        copies.append(pltpu.make_async_copy(acc_down.at[pl.ds(k * rows, rows)], g_down.at[k // RING, k % RING], sems.at[20 + k]))
    for copy in copies:
        copy.start()
    for copy in copies:
        copy.wait()


def gather_back(x, up, down, u_all, pre, act):
    vmem, anywhere = pl.BlockSpec(memory_space=pltpu.VMEM), pl.BlockSpec(memory_space=pl.ANY)
    hidden, width = x.shape[-1], up.shape[1]
    bf16, f32, dma = jnp.bfloat16, jnp.float32, pltpu.SemaphoreType.DMA
    return pl.pallas_call(
        back_kernel,
        out_shape=[jax.ShapeDtypeStruct(pre.shape, bf16),
                   jax.ShapeDtypeStruct((RING, RING) + up.shape, bf16),
                   jax.ShapeDtypeStruct((RING, RING, width, hidden // (RING * RING)), f32),
                   jax.ShapeDtypeStruct((RING, RING) + down.shape, f32)],
        in_specs=[vmem] * 3 + [anywhere] * 3,
        out_specs=[vmem] + [anywhere] * 3,
        scratch_shapes=[pltpu.VMEM((RING, CORES) + x.shape, bf16), pltpu.VMEM((RING, RING) + down.shape, bf16),
                        pltpu.VMEM(pre.shape[1:], f32), pltpu.VMEM(u_all.shape, bf16), pltpu.VMEM(pre.shape, bf16),
                        pltpu.VMEM(act.shape, bf16), pltpu.VMEM((width, hidden), f32), pltpu.VMEM((width, hidden), f32),
                        dma((Exchange.SLOTS,)), dma((Exchange.SLOTS,)), dma((36,))],
        compiler_params=pltpu.CompilerParams(collective_id=3, has_side_effects=True, vmem_limit_bytes=60 * 1024 * 1024),
        cost_estimate=pl.CostEstimate(flops=0, bytes_accessed=150_000_000, transcendentals=0),
        name="gather_back",
    )(x, up, down, u_all, pre, act)


def add_into(dst, *terms):
    if len(dst.shape) > 2:
        for i in range(dst.shape[0]):
            add_into(dst.at[i], *(term.at[i] for term in terms))
        return

    @pl.loop(0, dst.shape[0] // 8)
    def _(i):
        at = pl.ds(pl.multiple_of(i * 8, 8), 8)
        total = dst[at, :]
        for term in terms:
            total = total + term[at, :]
        dst[at, :] = total


class RingScatter:
    def __init__(self, sender, base, ring, block, relayed, arriving):
        self.s, self.base, self.block, self.relayed, self.arriving = sender, base, block, relayed, arriving
        self.me, self.right, self.left = ring
        self.prev, self.next = lax.rem(self.me + 3, RING), lax.rem(self.me + 1, RING)
        self.far = lax.rem(self.me + 2, RING)

    def start(self):
        self.s.start(self.base, self.block(self.far, 0), self.relayed(0), self.right)
        self.s.start(self.base + 1, self.block(self.far, 1), self.relayed(1), self.left)
        self.s.start(self.base + 2, self.block(self.next, 1), self.arriving(0, 1), self.right)
        self.s.start(self.base + 3, self.block(self.prev, 0), self.arriving(1, 0), self.left)

    def relay(self, to_next, to_prev):
        self.s.arrived(self.base, self.relayed(0), self.left)
        add_into(self.relayed(0), to_next)
        self.s.start(self.base + 4, self.relayed(0), self.arriving(0, 0), self.right)
        self.s.arrived(self.base + 1, self.relayed(1), self.right)
        add_into(self.relayed(1), to_prev)
        self.s.start(self.base + 5, self.relayed(1), self.arriving(1, 1), self.left)

    def finish(self):
        self.s.arrived(self.base + 2, self.arriving(0, 1), self.left)
        self.s.arrived(self.base + 3, self.arriving(1, 0), self.right)
        self.s.arrived(self.base + 4, self.arriving(0, 0), self.left)
        self.s.arrived(self.base + 5, self.arriving(1, 1), self.right)


class GradScatter:
    SLOTS = 24

    def __init__(self, p, sender, base, up, down, bufs, sems):
        self.p, self.sems, self.up, self.down = p, sems, up, down
        (self.u_rel, self.u_arr, self.u_loc, self.u_own, self.u_rel2, self.u_arr2,
         self.d_rel, self.d_arr, self.d_loc, self.d_own, self.d_rel2, self.d_arr2) = bufs
        ring_y, ring_z = p.along("y"), p.along("z")
        half = lambda h: pl.ds(2 * h, 2)
        u_rows, d_rows = up.shape[2] // 2, down.shape[2] // 2
        u_part, d_part = (lambda h: pl.ds(h * u_rows, u_rows)), (lambda h: pl.ds(h * d_rows, d_rows))
        self.up1 = RingScatter(sender, base, ring_y, lambda i, h: up.at[half(h), i], lambda h: self.u_rel.at[h],
                               lambda side, h: self.u_arr.at[side, half(h)])
        self.down1 = RingScatter(sender, base + 6, ring_z, lambda i, h: down.at[i, half(h)], lambda h: self.d_rel.at[h],
                                 lambda side, h: self.d_arr.at[side, half(h)])
        self.up2 = RingScatter(sender, base + 12, ring_z, lambda i, h: self.u_own.at[i, u_part(h)], lambda h: self.u_rel2.at[h],
                               lambda side, h: self.u_arr2.at[side, u_part(h)])
        self.down2 = RingScatter(sender, base + 18, ring_y, lambda i, h: self.d_own.at[i, d_part(h)], lambda h: self.d_rel2.at[h],
                                 lambda side, h: self.d_arr2.at[side, d_part(h)])
        self.u_part, self.d_part = u_part, d_part
        u, d = self.up1, self.down1
        pairs = [(up.at[half(0), u.next], self.u_loc.at[0]), (up.at[half(1), u.prev], self.u_loc.at[1]),
                 (up.at[:, u.me], self.u_own), (down.at[d.next, half(0)], self.d_loc.at[0]),
                 (down.at[d.prev, half(1)], self.d_loc.at[1]), (down.at[d.me], self.d_own)]
        self.loads = [pltpu.make_async_copy(src, dst, sems.at[k]) for k, (src, dst) in enumerate(pairs)]

    def load(self):
        for copy in self.loads:
            copy.start()

    def start(self):
        self.up1.start()
        self.down1.start()

    def relay(self):
        for copy in self.loads:
            copy.wait()
        self.up1.relay(self.u_loc.at[0], self.u_loc.at[1])
        self.down1.relay(self.d_loc.at[0], self.d_loc.at[1])

    def second(self):
        self.up1.finish()
        add_into(self.u_own, self.u_arr.at[0], self.u_arr.at[1])
        self.up2.start()
        self.down1.finish()
        add_into(self.d_own, self.d_arr.at[0], self.d_arr.at[1])
        self.down2.start()
        u, d = self.up2, self.down2
        u.relay(self.u_own.at[u.next, self.u_part(0)], self.u_own.at[u.prev, self.u_part(1)])
        d.relay(self.d_own.at[d.next, self.d_part(0)], self.d_own.at[d.prev, self.d_part(1)])

    def finish(self, up_out, down_out):
        self.up2.finish()
        self.down2.finish()
        up_out[...] = (self.u_own[self.up2.me] + self.u_arr2[0] + self.u_arr2[1]).T
        down_out[...] = self.d_own[self.down2.me] + self.d_arr2[0] + self.d_arr2[1]

    @staticmethod
    def buffers(up, down):
        f32 = jnp.float32
        out = []
        for rows, cols in (up.shape[2:], down.shape[2:]):
            out += [(2, 2, rows, cols), (2, RING, rows, cols), (2, 2, rows, cols), (RING, rows, cols),
                    (2, rows // 2, cols), (2, rows, cols)]
        return [pltpu.VMEM(shape, f32) for shape in out]


def scatter_kernel(h_ref, w_ref, *refs):
    backward = len(refs) > 8
    p = Place()
    me, right, left = p.along("x")
    sib, c, o = p.sibling(), p.core, 1 - p.core
    if backward:
        (g_up, g_down, y_ref, up_out, down_out, to_sib, from_sib, acc, relayed, arriving, send_sems, recv_sems,
         up_sum, local_sems, *bufs) = refs
        ring_y, ring_z = p.along("y"), p.along("z")
        others = [p.dev(x=lax.rem(me + dx, RING), core=lax.rem(c + dc, CORES)) for dx in range(RING) for dc in range(CORES)][1:]
        greet(others + [ring_y[1], ring_y[2], ring_z[1], ring_z[2]])
        s = Sender(send_sems, recv_sems)
        grads = GradScatter(p, s, 10, g_up, g_down, bufs, local_sems)
        grads.start()
        grads.load()
    else:
        y_ref, to_sib, from_sib, acc, relayed, arriving, send_sems, recv_sems = refs
        greet([right, left, sib])
        s = Sender(send_sems, recv_sems)
    hidden = y_ref.shape[1]
    rows = y_ref.shape[0] // 2
    step = 512
    first, second = pl.ds(0, rows), pl.ds(rows, rows)

    def product(dx, core, dst):
        block = lax.rem(me + dx, RING)

        @pl.loop(0, hidden // step)
        def _(n):
            at = pl.ds(pl.multiple_of(n * step, step), step)
            if backward:
                dst[:, at] = lax.dot_general(h_ref[block, core], w_ref[at, :], (((1,), (1,)), ((), ())),
                                             preferred_element_type=jnp.float32)
            else:
                dst[:, at] = jnp.dot(h_ref[block, core], w_ref[:, at], preferred_element_type=jnp.float32)

    def both(k, dx, dst):
        product(dx, o, to_sib.at[k])
        s.start(k, to_sib.at[k], from_sib.at[k], sib)
        product(dx, c, dst)

    def joined(k, dst):
        s.arrived(k, from_sib.at[k], sib)
        add_into(dst, from_sib.at[k])

    both(0, 2, acc.at[0])
    joined(0, acc.at[0])
    s.start(4, acc.at[0, first], relayed.at[0], right)
    s.start(5, acc.at[0, second], relayed.at[1], left)
    both(1, 1, acc.at[1])
    both(2, 3, acc.at[2])
    joined(1, acc.at[1])
    s.start(6, acc.at[1, second], arriving.at[0, second], right)
    joined(2, acc.at[2])
    s.start(7, acc.at[2, first], arriving.at[1, first], left)
    both(3, 0, y_ref)
    joined(3, y_ref)
    if backward:
        grads.relay()
    s.arrived(4, relayed.at[0], left)
    add_into(acc.at[1, first], relayed.at[0])
    s.start(8, acc.at[1, first], arriving.at[0, first], right)
    s.arrived(5, relayed.at[1], right)
    add_into(acc.at[2, second], relayed.at[1])
    s.start(9, acc.at[2, second], arriving.at[1, second], left)
    if backward:
        grads.second()
        grads.finish(up_sum, down_out)
        mine = me * CORES + c
        piece = up_out.shape[1]
        keep = pltpu.make_async_copy(up_sum.at[pl.ds(pl.multiple_of(mine * piece, piece), piece)], up_out.at[mine], local_sems.at[6])
        keep.start()
        turns = [(lax.rem(me + dx, RING), lax.rem(c + dc, CORES)) for dx in range(RING) for dc in range(CORES)][1:]
        for k, (x, core) in enumerate(turns):
            to = x * CORES + core
            s.start(34 + k, up_sum.at[pl.ds(pl.multiple_of(to * piece, piece), piece)], up_out.at[mine], p.dev(x=x, core=core))
    s.arrived(6, arriving.at[0, second], left)
    s.arrived(7, arriving.at[1, first], right)
    s.arrived(8, arriving.at[0, first], left)
    s.arrived(9, arriving.at[1, second], right)
    add_into(y_ref, arriving.at[0], arriving.at[1])
    if backward:
        for k in range(len(turns)):
            dx, dc = divmod(k + 1, CORES)
            x, core = lax.rem(me + RING - dx, RING), lax.rem(c + dc, CORES)
            s.arrived(34 + k, up_out.at[x * CORES + core], p.dev(x=x, core=core))
        keep.wait()
    s.drain()


def scatter(h, w, grads=None):
    rows, width = h.shape[2:]
    hidden = w.shape[1] if grads is None else w.shape[0]
    vmem, anywhere = pl.BlockSpec(memory_space=pltpu.VMEM), pl.BlockSpec(memory_space=pl.ANY)
    f32 = jnp.float32
    outs = [jax.ShapeDtypeStruct((rows, hidden), f32)]
    slots = 10
    extra = []
    if grads is not None:
        up_rows, down_rows = grads[0].shape[3], grads[1].shape[2]
        n_data = RING * CORES
        outs += [jax.ShapeDtypeStruct((n_data, up_rows // n_data, width), f32), jax.ShapeDtypeStruct((down_rows, hidden), f32)]
        slots = 10 + GradScatter.SLOTS + n_data - 1
        extra = [pltpu.VMEM((up_rows, width), f32), pltpu.SemaphoreType.DMA((7,))] + GradScatter.buffers(*grads)
    return pl.pallas_call(
        scatter_kernel,
        out_shape=outs,
        in_specs=[vmem] * 2 + [anywhere] * (0 if grads is None else 2),
        out_specs=[vmem] * len(outs),
        scratch_shapes=[pltpu.VMEM((RING, rows, hidden), f32), pltpu.VMEM((RING, rows, hidden), f32),
                        pltpu.VMEM((3, rows, hidden), f32), pltpu.VMEM((2, rows // 2, hidden), f32),
                        pltpu.VMEM((2, rows, hidden), f32),
                        pltpu.SemaphoreType.DMA((slots,)), pltpu.SemaphoreType.DMA((slots,))] + extra,
        compiler_params=pltpu.CompilerParams(collective_id=1 if grads is None else 2, has_side_effects=True,
                                             vmem_limit_bytes=(44 if grads is None else 62) * 1024 * 1024),
        cost_estimate=pl.CostEstimate(flops=0, bytes_accessed=240_000_000, transcendentals=0),
        name="scatter" if grads is None else "scatter_grads",
    )(h, w, *(grads or ()))


def solution(mesh):
    n_data = mesh.shape["data"]
    n_local = mesh.shape["local"]

    def body(tokens, cotangent, w_up, w_down):
        micro, rows, hidden = tokens.shape
        layers, up_rows, ffn = w_up.shape
        down_rows = w_down.shape[1]
        pad = PAD - down_rows
        width = n_local * PAD
        own = micro * rows

        up = w_up.reshape(layers, up_rows, n_local, n_data, down_rows)
        up = jnp.pad(up, ((0, 0),) * 4 + ((0, pad),))
        up = up.transpose(3, 0, 1, 2, 4).reshape(n_data, layers, up_rows, width)
        up = lax.all_to_all(up, "data", 0, 0)
        up = up.transpose(1, 0, 2, 3).reshape(layers, n_data * up_rows, width)
        down = jnp.pad(w_down, ((0, 0), (0, pad), (0, 0)))

        def shaped(x):
            return x.reshape(micro, rows, hidden)

        def blocks(h):
            return h.reshape(RING, CORES, own, width)

        x_cur = tokens.reshape(own, hidden)
        saved = []
        for layer in range(layers):
            x_f32 = x_cur.astype(jnp.float32)
            normed = norm_f32(x_f32).astype(jnp.bfloat16)
            u_all, pre, act, w2 = gather_up(shaped(normed), up[layer], down[layer])
            y, = scatter(blocks(act), w2.reshape(width, hidden))
            saved.append((x_cur, u_all, pre, act))
            x_cur = (x_f32 + y).astype(jnp.bfloat16)
        x_final = x_cur

        d_cur = cotangent.reshape(own, hidden)
        d_cur, x_final = lax.optimization_barrier((d_cur, x_final))
        grads_up = [None] * layers
        grads_down = [None] * layers
        for layer in reversed(range(layers)):
            x_in, u_all, pre, act = saved[layer]
            z, w1, g_up, g_down = gather_back(shaped(d_cur), up[layer], down[layer], u_all, pre, act)
            v, grads_up[layer], g_down = scatter(blocks(z), w1.reshape(hidden, width), (g_up, g_down))
            grads_down[layer] = g_down[:down_rows]
            norm_pull = jax.vjp(norm_f32, x_in.astype(jnp.float32))[1]
            d_cur = (d_cur.astype(jnp.float32) + norm_pull(v)[0]).astype(jnp.bfloat16)
        g_up = jnp.stack(grads_up, 1).reshape(n_data, layers, up_rows, n_local, PAD)[..., :down_rows]
        g_up = g_up.transpose(1, 2, 3, 0, 4).reshape(layers, up_rows, ffn)
        shape = (micro, rows, hidden)
        return x_final.reshape(shape), d_cur.reshape(shape), g_up, jnp.stack(grads_down)

    spec = P(None, ALL_AXES, None)
    return jax.shard_map(body, mesh=mesh, in_specs=(spec,) * 4, out_specs=(spec,) * 4, check_vma=False)
```

```python
import functools

import jax
import jax.numpy as jnp
from jax import lax
from jax.experimental import pallas as pl
from jax.experimental.pallas import tpu as pltpu
from jax.sharding import PartitionSpec as P

NORM_EPS = 1e-6
ALL_AXES = ("local", "data")
PAD = 48
RING = 4
CORES = 2
HALVES = (0, 1)
VMEM = 62 * 2**20
ROWS = (((1,), (1,)), ((), ()))
MESH = pl.DeviceIdType.MESH


def norm_f32(x_f32):
    return x_f32 * lax.rsqrt(jnp.mean(x_f32 * x_f32, axis=-1, keepdims=True) + NORM_EPS)


def gelu_f32(pre_f32):
    return jax.nn.gelu(pre_f32, approximate=True)


class Place:
    def __init__(self):
        local, data = lax.axis_index("local"), lax.axis_index("data")
        self.z, self.y = local // RING, local % RING
        self.x, self.core = data // CORES, data % CORES

    def dev(self, **at):
        z, y, x, core = (at.get(name, getattr(self, name)) for name in ("z", "y", "x", "core"))
        return (z * RING + y, x * CORES + core)

    def along(self, axis):
        me = getattr(self, axis)
        left, right, _ = around(me)
        return me, self.dev(**{axis: right}), self.dev(**{axis: left})

    def sibling(self):
        return self.dev(core=1 - self.core)


def around(me):
    return [lax.rem(me + k, RING) for k in (3, 1, 2)]


def greet(devices):
    barrier = pltpu.get_barrier_semaphore()
    for device in devices:
        pl.semaphore_signal(barrier, inc=1, device_id=device, device_id_type=MESH)
    pl.semaphore_wait(barrier, len(devices))


class Sender:
    def __init__(self, send_sems, recv_sems):
        self.send_sems, self.recv_sems, self.started = send_sems, recv_sems, []

    def copy(self, slot, src, dst, device, there=None):
        there = slot if there is None else there
        c = pltpu.make_async_remote_copy(src_ref=src, dst_ref=dst, send_sem=self.send_sems.at[slot],
                                         recv_sem=self.recv_sems.at[there], device_id=device, device_id_type=MESH)
        return c

    def start(self, slot, src, dst, device, there=None):
        c = self.copy(slot, src, dst, device, there)
        c.start()
        self.started.append(c)

    def arrived(self, slot, dst, device):
        self.copy(0, dst, dst, device, slot).wait_recv()

    def drain(self):
        for c in self.started:
            c.wait_send()


class RingGather:
    def __init__(self, sender, base, ring, own, block):
        self.s, self.base, self.own, self.block = sender, base, own, block
        self.me, self.right, self.left = ring
        self.prev, self.next, self.far = around(self.me)

    def start(self, halves=HALVES):
        for h in halves:
            self.s.start(self.base + h, self.own(h), self.block(self.me, h), self.right)
            self.s.start(self.base + 3 - h, self.own(1 - h), self.block(self.me, 1 - h), self.left)

    def relay(self):
        self.s.arrived(self.base, self.block(self.prev, 0), self.left)
        self.s.start(self.base + 4, self.block(self.prev, 0), self.block(self.prev, 0), self.right)
        self.s.arrived(self.base + 3, self.block(self.next, 1), self.right)
        self.s.start(self.base + 5, self.block(self.next, 1), self.block(self.next, 1), self.left)

    def near(self):
        self.s.arrived(self.base + 1, self.block(self.prev, 1), self.left)
        self.s.arrived(self.base + 2, self.block(self.next, 0), self.right)

    def finish(self):
        self.s.arrived(self.base + 4, self.block(self.far, 0), self.left)
        self.s.arrived(self.base + 5, self.block(self.far, 1), self.right)


class WeightGather:
    def __init__(self, p, sender, base, src, dst):
        ring_y, ring_z = p.along("y"), p.along("z")
        rows, cols = src.shape
        if rows >= 64:
            quarter = rows // 4
            sub = lambda part, h: (pl.ds((2 * part + h) * quarter, quarter), slice(None))
        else:
            quarter = cols // 4
            sub = lambda part, h: (slice(None), pl.ds((2 * part + h) * quarter, quarter))
        block2 = (lambda i, h: dst.at[(i, slice(None)) + sub(0, h)], lambda i, h: dst.at[(slice(None), i) + sub(1, h)])
        self.block2 = block2
        self.stage1 = (RingGather(sender, base, ring_y, lambda h: src.at[sub(0, h)], lambda i, h: dst.at[(p.z, i) + sub(0, h)]),
                       RingGather(sender, base + 6, ring_z, lambda h: src.at[sub(1, h)], lambda i, h: dst.at[(i, p.y) + sub(1, h)]))
        self.stage2 = (RingGather(sender, base + 12, ring_z, lambda h: block2[0](p.z, h), block2[0]),
                       RingGather(sender, base + 18, ring_y, lambda h: block2[1](p.y, h), block2[1]))

    def start(self):
        for g in self.stage1:
            g.start()

    def second(self, keep=None):
        self.early()
        self.late(keep)

    def early(self):
        for g in self.stage1:
            g.relay()

    def late(self, keep=None):
        for g in self.stage1:
            g.near()
            g.finish()
        if keep is not None:
            keep.wait()
        for g in self.stage2:
            g.start()

    def relay(self):
        for g in self.stage2:
            g.relay()

    def finish(self):
        for g in self.stage2:
            g.near()
            g.finish()


class Exchange:
    SLOTS = 62

    def __init__(self, x_ref, xs, first, first_dst, second, second_dst, send_sems, recv_sems, keep_sem):
        p = Place()
        ring_x, ring_y, ring_z = p.along("x"), p.along("y"), p.along("z")
        self.p, self.sib, self.xs, self.x_ref = p, p.sibling(), xs, x_ref
        c = p.core
        self.keep = pltpu.make_async_copy(second, second_dst.at[p.z, p.y], keep_sem)
        self.keep.start()
        first_dst[p.z, p.y] = first[...]
        xs[p.x, c] = x_ref[...]
        greet([ring_x[1], ring_x[2], ring_y[1], ring_y[2], ring_z[1], ring_z[2], self.sib])
        self.s = Sender(send_sems, recv_sems)
        self.gx = RingGather(self.s, 0, ring_x, lambda h: x_ref.at[h], lambda i, h: xs.at[i, c, h])
        self.first = WeightGather(p, self.s, 14, first, first_dst)
        self.second = WeightGather(p, self.s, 38, second, second_dst)

    def give(self, k, i, h, src=None):
        at = self.xs.at[i, self.p.core, h]
        self.s.start(6 + k, at if src is None else src, at, self.sib)

    def take(self, k, i, h):
        self.s.arrived(6 + k, self.xs.at[i, 1 - self.p.core, h], self.sib)

    def run(self, early, compute):
        gx, me = self.gx, self.p.x
        self.first.start()
        gx.start()
        for h in HALVES:
            self.give(h, me, h, self.x_ref.at[h])
        self.second.start()
        self.first.second()
        self.second.early()
        for h in HALVES:
            self.take(h, me, h)
        early(me, True)
        gx.relay()
        self.give(2, gx.prev, 0)
        self.give(3, gx.next, 1)
        self.first.relay()
        self.second.late(self.keep)
        self.first.finish()
        compute(me, True)
        gx.near()
        self.give(4, gx.prev, 1)
        self.give(5, gx.next, 0)
        self.take(2, gx.prev, 0)
        self.take(4, gx.prev, 1)
        self.second.relay()
        early(gx.prev, False)
        compute(gx.prev, False)
        self.take(3, gx.next, 1)
        self.take(5, gx.next, 0)
        gx.finish()
        self.give(6, gx.far, 0)
        self.give(7, gx.far, 1)
        early(gx.next, False)
        compute(gx.next, False)
        self.take(6, gx.far, 0)
        self.take(7, gx.far, 1)
        early(gx.far, False, True)
        compute(gx.far, False)
        self.second.finish()
        self.s.drain()


def forward_kernel(x_ref, up_ref, down_ref, u_ref, slope_ref, act_ref, y_ref, xs, w1, wide, shards, w2, acts, passing,
                   send_sems, recv_sems, sems):
    p = Place()
    me, right, left = p.along("x")
    ring_y, ring_z = p.along("y"), p.along("z")
    c, o, sib = p.core, 1 - p.core, p.sibling()
    hidden, width = xs.shape[-1], w1.shape[-1]
    rows, half_cols = down_ref.shape[0], down_ref.shape[1] // 2
    own = acts.shape[2]
    half = own // 2
    mine = pl.ds(pl.multiple_of(me * rows, 16), rows)
    w1[p.z, p.y] = up_ref[...]
    shards[mine, :] = down_ref[...]
    xs[me, c] = x_ref[...]
    prev, next_, far = around(me)
    greet([right, left, p.dev(x=prev, core=o), p.dev(x=next_, core=o), ring_y[1], ring_y[2], ring_z[1], ring_z[2], sib])
    s = Sender(send_sems, recv_sems)
    gx = RingGather(s, 0, (me, right, left), lambda h: x_ref.at[h], lambda i, h: xs.at[i, c, h])
    gd = RingGather(s, 6, (me, right, left), lambda h: down_ref.at[:, pl.ds(h * half_cols, half_cols)],
                    lambda i, h: shards.at[pl.ds(pl.multiple_of(i * rows, 16), rows), pl.ds(h * half_cols, half_cols)])
    up = WeightGather(p, s, 12, up_ref, w1)
    down = WeightGather(p, s, 36, shards, w2.at[c])
    down_there = WeightGather(p, s, 36, shards, w2.at[o])
    saves = []

    def give(k, i, h, src=None):
        at = xs.at[i, c, h]
        s.start(60 + k, at if src is None else src, at, sib)

    def take(k, i, h):
        s.arrived(60 + k, xs.at[i, o, h], sib)

    def rings():
        for part, ring in enumerate(down.stage2):
            yield part, ring

    def share(which):
        for part, ring in rings():
            for h in HALVES:
                if which == "own":
                    i, k = ring.me, 0
                elif which == "relayed":
                    i, k = (ring.prev, 1) if h == 0 else (ring.next, 2)
                elif which == "near":
                    i, k = (ring.next, 2) if h == 0 else (ring.prev, 1)
                else:
                    i, k = ring.far, 3
                at = down.block2[part](i, h)
                s.start(68 + part * 8 + k * 2 + h, at, at, sib)

    def shared():
        for part, ring in rings():
            for k, i in enumerate((ring.me, ring.prev, ring.next, ring.far)):
                for h in HALVES:
                    s.arrived(68 + part * 8 + k * 2 + h, down_there.block2[part](i, h), sib)

    def save(src, dst):
        copy = pltpu.make_async_copy(src, dst, sems.at[len(saves)])
        copy.start()
        saves.append(copy)

    def compute(i):
        if saves:
            saves[-1].wait()
        save(xs.at[i], u_ref.at[i])
        wide[...] = jnp.dot(xs[i].reshape(wide.shape[0], hidden), w1[...].reshape(hidden, width),
                            preferred_element_type=jnp.float32)

        @pl.loop(0, wide.shape[0] // 32)
        def _(r):
            at = pl.ds(pl.multiple_of(r * 32, 32), 32)
            act, pull = jax.vjp(gelu_f32, wide[at, :].astype(jnp.bfloat16).astype(jnp.float32))
            act_ref[i, at, :] = act.astype(jnp.bfloat16)
            wide[at, :] = pull(jnp.ones_like(act))[0]

        save(wide, slope_ref.at[i])

    def rows_of(core, h=None):
        if h is None:
            return pl.ds(pl.multiple_of(core * own, own), own)
        return pl.ds(core * own + h * half, half)

    def send_act(k, i, to_right):
        for core in HALVES:
            s.start(k + core, act_ref.at[i, rows_of(core)], acts.at[me, c], p.dev(x=i, core=core),
                    there=(85 if to_right else 87) + c)

    gd.start()
    up.start()
    gd.relay()
    gx.start()
    for h in HALVES:
        give(h, me, h, x_ref.at[h])
    up.second()
    gd.near()
    gd.finish()
    w2[c, p.z, p.y] = shards[...]
    up.relay()
    down.start()
    gx.relay()
    give(2, prev, 0)
    give(3, next_, 1)
    up.finish()
    take(0, me, 0)
    take(1, me, 1)
    compute(me)
    s.start(84, act_ref.at[me, rows_of(o)], acts.at[me, c], sib)
    acts[me, c] = act_ref[me, rows_of(c), :]
    down.early()
    gx.near()
    give(4, prev, 1)
    give(5, next_, 0)
    take(2, prev, 0)
    take(4, prev, 1)
    compute(prev)
    send_act(85, prev, False)
    down.late()
    share("own")
    take(3, next_, 1)
    take(5, next_, 0)
    compute(next_)
    send_act(87, next_, True)
    gx.finish()
    give(6, far, 0)
    give(7, far, 1)
    take(6, far, 0)
    take(7, far, 1)
    compute(far)
    for core in HALVES:
        s.start(89 + core, act_ref.at[far, rows_of(core, 0)], passing.at[0, core], right)
        s.start(91 + core, act_ref.at[far, rows_of(core, 1)], passing.at[1, core], left)
    down.relay()
    share("relayed")
    for core in HALVES:
        s.arrived(89 + core, passing.at[0, core], left)
        s.start(93 + core, passing.at[0, core], acts.at[prev, c, pl.ds(0, half)], p.dev(x=next_, core=core), there=93 + c)
        s.arrived(91 + core, passing.at[1, core], right)
        s.start(95 + core, passing.at[1, core], acts.at[next_, c, pl.ds(half, half)], p.dev(x=prev, core=core), there=95 + c)
    for ring in down.stage2:
        ring.near()
    share("near")
    s.arrived(84, acts.at[me, o], sib)
    for core in HALVES:
        s.arrived(85 + core, acts.at[prev, core], left)
        s.arrived(87 + core, acts.at[next_, core], right)
        s.arrived(93 + core, acts.at[far, core, pl.ds(0, half)], left)
        s.arrived(95 + core, acts.at[far, core, pl.ds(half, half)], right)
    for ring in down.stage2:
        ring.finish()
    share("far")

    def product(core, initial):
        step = 512

        @pl.loop(0, hidden // step)
        def _(n):
            at = pl.ds(pl.multiple_of(n * step, step), step)
            total = None
            for x in range(RING):
                w = w2.at[core, :, :, pl.ds(x * rows, rows), at][...].reshape(width, step)
                term = jnp.dot(acts[x, core], w, preferred_element_type=jnp.float32)
                total = term if total is None else total + term
            if initial:
                y_ref[:, at] = total
            else:
                y_ref[:, at] += total

    product(c, True)
    shared()
    product(o, False)
    for copy in saves[::2] + saves[-1:]:
        copy.wait()
    s.drain()


def forward(x, up, down):
    vmem, anywhere = pl.BlockSpec(memory_space=pltpu.VMEM), pl.BlockSpec(memory_space=pl.ANY)
    micro, rows, hidden = x.shape
    own, width = micro * rows, up.shape[1]
    block = CORES * own
    bf16, f32, dma = jnp.bfloat16, jnp.float32, pltpu.SemaphoreType.DMA
    shards = (RING * down.shape[0], hidden)
    return pl.pallas_call(
        forward_kernel,
        out_shape=[jax.ShapeDtypeStruct((RING, CORES) + x.shape, bf16), jax.ShapeDtypeStruct((RING, block, width), f32),
                   jax.ShapeDtypeStruct((RING, block, width), bf16), jax.ShapeDtypeStruct((own, hidden), f32)],
        in_specs=[vmem] * 3,
        out_specs=[anywhere, anywhere, vmem, vmem],
        scratch_shapes=[pltpu.VMEM((RING, CORES) + x.shape, bf16), pltpu.VMEM((RING, RING) + up.shape, bf16),
                        pltpu.VMEM((block, width), f32), pltpu.VMEM(shards, bf16),
                        pltpu.VMEM((CORES, RING, RING) + shards, bf16), pltpu.VMEM((RING, CORES, own, width), bf16),
                        pltpu.VMEM((2, CORES, own // 2, width), bf16), dma((97,)), dma((97,)), dma((8,))],
        compiler_params=pltpu.CompilerParams(collective_id=0, has_side_effects=True, vmem_limit_bytes=VMEM),
        name="forward",
    )(x, up, down)


def back_kernel(x_ref, up_ref, down_ref, u_hbm, slope_hbm, act_hbm, z_ref, w1_ref, g_up, g_down,
                xs, w2, wide, us, slopes, acts, acc_up, acc_down, flipped, send_sems, recv_sems, sems):
    loads = [pltpu.make_async_copy(src, dst, sems.at[1 + k])
             for k, (src, dst) in enumerate(((slope_hbm, slopes), (act_hbm, acts), (u_hbm, us)))]
    for load in loads:
        load.start()
    hidden, width = xs.shape[-1], z_ref.shape[-1]
    block = wide.shape[0]
    ex = Exchange(x_ref, xs, down_ref, w2, up_ref, w1_ref, send_sems, recv_sems, sems.at[0])
    step = 512

    def accumulate(acc, left, right, i, initial):
        flipped[...] = left[i].T

        @pl.loop(0, hidden // step)
        def _(n):
            at = pl.ds(pl.multiple_of(n * step, step), step)
            term = jnp.dot(flipped[...], right.at[i, :, :, :, at][...].reshape(block, step), preferred_element_type=jnp.float32)
            if initial:
                acc[:, at] = term
            else:
                acc[:, at] += term

    cols, rows = g_up.shape[3], g_down.shape[2]
    copies = []

    def store(acc_at, grad, base):
        for k in range(RING * RING):
            copy = pltpu.make_async_copy(acc_at(k), grad.at[k // RING, k % RING], sems.at[base + k])
            copy.start()
            copies.append(copy)

    def early(i, initial, last=False):
        if initial:
            for load in loads:
                load.wait()
        accumulate(acc_down, acts, xs, i, initial)
        if last:
            store(lambda k: acc_down.at[pl.ds(k * rows, rows)], g_down, 4)

    def compute(i, initial):
        wide[...] = lax.dot_general(xs[i].reshape(block, hidden), w2[...].reshape(width, hidden), ROWS,
                                    preferred_element_type=jnp.float32)

        @pl.loop(0, block // 32)
        def _(r):
            at = pl.ds(pl.multiple_of(r * 32, 32), 32)
            z_ref[i, at, :] = (wide[at, :] * slopes[i, at, :]).astype(jnp.bfloat16)

        accumulate(acc_up, z_ref, us, i, initial)

    ex.run(early, compute)
    store(lambda k: acc_up.at[:, pl.ds(k * cols, cols)], g_up, 20)
    for copy in copies:
        copy.wait()


def gather_back(x, up, down, u_all, slope, act):
    vmem, anywhere = pl.BlockSpec(memory_space=pltpu.VMEM), pl.BlockSpec(memory_space=pl.ANY)
    hidden, width = x.shape[-1], up.shape[1]
    bf16, f32, dma = jnp.bfloat16, jnp.float32, pltpu.SemaphoreType.DMA
    return pl.pallas_call(
        back_kernel,
        out_shape=[jax.ShapeDtypeStruct(act.shape, bf16),
                   jax.ShapeDtypeStruct((RING, RING) + up.shape, bf16),
                   jax.ShapeDtypeStruct((RING, RING, width, hidden // (RING * RING)), f32),
                   jax.ShapeDtypeStruct((RING, RING) + down.shape, f32)],
        in_specs=[vmem] * 3 + [anywhere] * 3,
        out_specs=[vmem] + [anywhere] * 3,
        scratch_shapes=[pltpu.VMEM((RING, CORES) + x.shape, bf16), pltpu.VMEM((RING, RING) + down.shape, bf16),
                        pltpu.VMEM(slope.shape[1:], f32), pltpu.VMEM(u_all.shape, bf16), pltpu.VMEM(slope.shape, f32),
                        pltpu.VMEM(act.shape, bf16), pltpu.VMEM((width, hidden), f32), pltpu.VMEM((width, hidden), f32),
                        pltpu.VMEM(act.shape[:0:-1], bf16),
                        dma((Exchange.SLOTS,)), dma((Exchange.SLOTS,)), dma((36,))],
        compiler_params=pltpu.CompilerParams(collective_id=3, has_side_effects=True, vmem_limit_bytes=VMEM),
        name="gather_back",
    )(x, up, down, u_all, slope, act)


def add_into(dst, *terms):
    if len(dst.shape) > 2:
        for i in range(dst.shape[0]):
            add_into(dst.at[i], *(term.at[i] for term in terms))
        return

    @pl.loop(0, dst.shape[0] // 8)
    def _(i):
        at = pl.ds(pl.multiple_of(i * 8, 8), 8)
        total = dst[at, :]
        for term in terms:
            total = total + term[at, :]
        dst[at, :] = total


class RingScatter:
    def __init__(self, sender, base, ring, block, relayed, arriving):
        self.s, self.base, self.block, self.relayed, self.arriving = sender, base, block, relayed, arriving
        self.me, self.right, self.left = ring
        self.prev, self.next, self.far = around(self.me)

    def start(self):
        self.s.start(self.base, self.block(self.far, 0), self.relayed(0), self.right)
        self.s.start(self.base + 1, self.block(self.far, 1), self.relayed(1), self.left)
        self.s.start(self.base + 2, self.block(self.next, 1), self.arriving(0, 1), self.right)
        self.s.start(self.base + 3, self.block(self.prev, 0), self.arriving(1, 0), self.left)

    def relay(self, to_next, to_prev):
        self.s.arrived(self.base, self.relayed(0), self.left)
        add_into(self.relayed(0), to_next)
        self.s.start(self.base + 4, self.relayed(0), self.arriving(0, 0), self.right)
        self.s.arrived(self.base + 1, self.relayed(1), self.right)
        add_into(self.relayed(1), to_prev)
        self.s.start(self.base + 5, self.relayed(1), self.arriving(1, 1), self.left)

    def finish(self):
        self.s.arrived(self.base + 2, self.arriving(0, 1), self.left)
        self.s.arrived(self.base + 3, self.arriving(1, 0), self.right)
        self.s.arrived(self.base + 4, self.arriving(0, 0), self.left)
        self.s.arrived(self.base + 5, self.arriving(1, 1), self.right)


class GradScatter:
    SLOTS = 24

    def __init__(self, p, sender, base, up, down, bufs, sems):
        self.p, self.sems, self.up, self.down = p, sems, up, down
        (self.u_rel, self.u_arr, self.u_loc, self.u_own, self.u_rel2, self.u_arr2,
         self.d_rel, self.d_arr, self.d_loc, self.d_own, self.d_rel2, self.d_arr2) = bufs
        ring_y, ring_z = p.along("y"), p.along("z")
        half = lambda h: pl.ds(2 * h, 2)
        u_rows, d_rows = up.shape[2] // 2, down.shape[2] // 2
        u_part, d_part = (lambda h: pl.ds(h * u_rows, u_rows)), (lambda h: pl.ds(h * d_rows, d_rows))
        self.up1 = RingScatter(sender, base, ring_y, lambda i, h: up.at[half(h), i], lambda h: self.u_rel.at[h],
                               lambda side, h: self.u_arr.at[side, half(h)])
        self.down1 = RingScatter(sender, base + 6, ring_z, lambda i, h: down.at[i, half(h)], lambda h: self.d_rel.at[h],
                                 lambda side, h: self.d_arr.at[side, half(h)])
        self.up2 = RingScatter(sender, base + 12, ring_z, lambda i, h: self.u_own.at[i, u_part(h)], lambda h: self.u_rel2.at[h],
                               lambda side, h: self.u_arr2.at[side, u_part(h)])
        self.down2 = RingScatter(sender, base + 18, ring_y, lambda i, h: self.d_own.at[i, d_part(h)], lambda h: self.d_rel2.at[h],
                                 lambda side, h: self.d_arr2.at[side, d_part(h)])
        self.u_part, self.d_part = u_part, d_part
        u, d = self.up1, self.down1
        pairs = [(up.at[half(0), u.next], self.u_loc.at[0]), (up.at[half(1), u.prev], self.u_loc.at[1]),
                 (up.at[:, u.me], self.u_own), (down.at[d.next, half(0)], self.d_loc.at[0]),
                 (down.at[d.prev, half(1)], self.d_loc.at[1]), (down.at[d.me], self.d_own)]
        self.loads = [pltpu.make_async_copy(src, dst, sems.at[k]) for k, (src, dst) in enumerate(pairs)]

    def load(self):
        for copy in self.loads:
            copy.start()

    def start(self):
        self.up1.start()
        self.down1.start()

    def relay(self):
        for copy in self.loads:
            copy.wait()
        self.up1.relay(self.u_loc.at[0], self.u_loc.at[1])
        self.down1.relay(self.d_loc.at[0], self.d_loc.at[1])

    def second(self):
        self.up1.finish()
        add_into(self.u_own, self.u_arr.at[0], self.u_arr.at[1])
        self.up2.start()
        self.down1.finish()
        add_into(self.d_own, self.d_arr.at[0], self.d_arr.at[1])
        self.down2.start()
        u, d = self.up2, self.down2
        u.relay(self.u_own.at[u.next, self.u_part(0)], self.u_own.at[u.prev, self.u_part(1)])
        d.relay(self.d_own.at[d.next, self.d_part(0)], self.d_own.at[d.prev, self.d_part(1)])

    def finish(self, up_out, down_out):
        self.up2.finish()
        self.down2.finish()
        up_out[...] = (self.u_own[self.up2.me] + self.u_arr2[0] + self.u_arr2[1]).T
        down_out[...] = self.d_own[self.down2.me] + self.d_arr2[0] + self.d_arr2[1]

    @staticmethod
    def buffers(up, down):
        f32 = jnp.float32
        out = []
        for rows, cols in (up.shape[2:], down.shape[2:]):
            out += [(2, 2, rows, cols), (2, RING, rows, cols), (2, 2, rows, cols), (RING, rows, cols),
                    (2, rows // 2, cols), (2, rows, cols)]
        return [pltpu.VMEM(shape, f32) for shape in out]


def scatter_kernel(h_ref, w_ref, *refs):
    p = Place()
    me, right, left = p.along("x")
    sib, c, o = p.sibling(), p.core, 1 - p.core
    (g_up, g_down, y_ref, up_out, down_out, to_sib, from_sib, acc, relayed, arriving, send_sems, recv_sems,
     up_sum, local_sems, *bufs) = refs
    ring_y, ring_z = p.along("y"), p.along("z")
    turns = [(lax.rem(me + dx, RING), lax.rem(c + dc, CORES)) for dx in range(RING) for dc in range(CORES)][1:]
    greet([p.dev(x=x, core=core) for x, core in turns] + [ring_y[1], ring_y[2], ring_z[1], ring_z[2]])
    s = Sender(send_sems, recv_sems)
    grads = GradScatter(p, s, 10, g_up, g_down, bufs, local_sems)
    grads.start()
    grads.load()
    hidden = y_ref.shape[1]
    rows = y_ref.shape[0] // 2
    step = 512
    first, second = pl.ds(0, rows), pl.ds(rows, rows)

    def product(dx, core, dst):
        block = lax.rem(me + dx, RING)

        @pl.loop(0, hidden // step)
        def _(n):
            at = pl.ds(pl.multiple_of(n * step, step), step)
            dst[:, at] = lax.dot_general(h_ref[block, core], w_ref[at, :], ROWS,
                                         preferred_element_type=jnp.float32)

    def both(k, dx, dst):
        product(dx, o, to_sib.at[k])
        s.start(k, to_sib.at[k], from_sib.at[k], sib)
        product(dx, c, dst)

    def joined(k, dst):
        s.arrived(k, from_sib.at[k], sib)
        add_into(dst, from_sib.at[k])

    both(0, 2, acc.at[0])
    joined(0, acc.at[0])
    s.start(4, acc.at[0, first], relayed.at[0], right)
    s.start(5, acc.at[0, second], relayed.at[1], left)
    both(1, 1, acc.at[1])
    both(2, 3, acc.at[2])
    joined(1, acc.at[1])
    s.start(6, acc.at[1, second], arriving.at[0, second], right)
    joined(2, acc.at[2])
    s.start(7, acc.at[2, first], arriving.at[1, first], left)
    both(3, 0, y_ref)
    joined(3, y_ref)
    grads.relay()
    s.arrived(4, relayed.at[0], left)
    add_into(acc.at[1, first], relayed.at[0])
    s.start(8, acc.at[1, first], arriving.at[0, first], right)
    s.arrived(5, relayed.at[1], right)
    add_into(acc.at[2, second], relayed.at[1])
    s.start(9, acc.at[2, second], arriving.at[1, second], left)
    grads.second()
    grads.finish(up_sum, down_out)
    mine = me * CORES + c
    piece = up_out.shape[1]
    keep = pltpu.make_async_copy(up_sum.at[pl.ds(pl.multiple_of(mine * piece, piece), piece)], up_out.at[mine], local_sems.at[6])
    keep.start()
    for k, (x, core) in enumerate(turns):
        to = x * CORES + core
        s.start(34 + k, up_sum.at[pl.ds(pl.multiple_of(to * piece, piece), piece)], up_out.at[mine], p.dev(x=x, core=core))
    s.arrived(6, arriving.at[0, second], left)
    s.arrived(7, arriving.at[1, first], right)
    s.arrived(8, arriving.at[0, first], left)
    s.arrived(9, arriving.at[1, second], right)
    add_into(y_ref, arriving.at[0], arriving.at[1])
    for k in range(len(turns)):
        dx, dc = divmod(k + 1, CORES)
        x, core = lax.rem(me + RING - dx, RING), lax.rem(c + dc, CORES)
        s.arrived(34 + k, up_out.at[x * CORES + core], p.dev(x=x, core=core))
    keep.wait()
    s.drain()


def scatter(h, w, grads):
    rows, width = h.shape[2:]
    hidden = w.shape[0]
    vmem, anywhere = pl.BlockSpec(memory_space=pltpu.VMEM), pl.BlockSpec(memory_space=pl.ANY)
    f32 = jnp.float32
    up_rows, down_rows = grads[0].shape[3], grads[1].shape[2]
    n_data = RING * CORES
    slots = 10 + GradScatter.SLOTS + n_data - 1
    return pl.pallas_call(
        scatter_kernel,
        out_shape=[jax.ShapeDtypeStruct((rows, hidden), f32),
                   jax.ShapeDtypeStruct((n_data, up_rows // n_data, width), f32), jax.ShapeDtypeStruct((down_rows, hidden), f32)],
        in_specs=[vmem] * 2 + [anywhere] * 2,
        out_specs=[vmem] * 3,
        scratch_shapes=[pltpu.VMEM((RING, rows, hidden), f32), pltpu.VMEM((RING, rows, hidden), f32),
                        pltpu.VMEM((3, rows, hidden), f32), pltpu.VMEM((2, rows // 2, hidden), f32),
                        pltpu.VMEM((2, rows, hidden), f32),
                        pltpu.SemaphoreType.DMA((slots,)), pltpu.SemaphoreType.DMA((slots,)),
                        pltpu.VMEM((up_rows, width), f32), pltpu.SemaphoreType.DMA((7,))] + GradScatter.buffers(*grads),
        compiler_params=pltpu.CompilerParams(collective_id=2, has_side_effects=True, vmem_limit_bytes=VMEM),
        name="scatter_grads",
    )(h, w, *grads)


def solution(mesh):
    n_data = mesh.shape["data"]
    n_local = mesh.shape["local"]

    def body(tokens, cotangent, w_up, w_down):
        micro, rows, hidden = tokens.shape
        layers, up_rows, ffn = w_up.shape
        down_rows = w_down.shape[1]
        pad = PAD - down_rows
        width = n_local * PAD
        own = micro * rows

        up = w_up.reshape(layers, up_rows, n_local, n_data, down_rows)
        up = jnp.pad(up, ((0, 0),) * 4 + ((0, pad),))
        up = up.transpose(3, 0, 1, 2, 4).reshape(n_data, layers, up_rows, width)
        up = lax.all_to_all(up, "data", 0, 0)
        up = up.transpose(1, 0, 2, 3).reshape(layers, n_data * up_rows, width)
        down = jnp.pad(w_down, ((0, 0), (0, pad), (0, 0)))

        def shaped(x):
            return x.reshape(micro, rows, hidden)

        def blocks(h):
            return h.reshape(RING, CORES, own, width)

        x_cur = tokens.reshape(own, hidden)
        saved = []
        for layer in range(layers):
            x_f32 = x_cur.astype(jnp.float32)
            normed = norm_f32(x_f32).astype(jnp.bfloat16)
            u_all, slope, act, y = forward(shaped(normed), up[layer], down[layer])
            saved.append((x_cur, u_all, slope, act))
            x_cur = (x_f32 + y).astype(jnp.bfloat16)
        x_final = x_cur

        d_cur = cotangent.reshape(own, hidden)
        d_cur, x_final = lax.optimization_barrier((d_cur, x_final))
        grads_up = [None] * layers
        grads_down = [None] * layers
        for layer in reversed(range(layers)):
            x_in, u_all, slope, act = saved[layer]
            z, w1, g_up, g_down = gather_back(shaped(d_cur), up[layer], down[layer], u_all, slope, act)
            v, grads_up[layer], g_down = scatter(blocks(z), w1.reshape(hidden, width), (g_up, g_down))
            grads_down[layer] = g_down[:down_rows]
            norm_pull = jax.vjp(norm_f32, x_in.astype(jnp.float32))[1]
            d_cur = (d_cur.astype(jnp.float32) + norm_pull(v)[0]).astype(jnp.bfloat16)
        g_up = jnp.stack(grads_up, 1).reshape(n_data, layers, up_rows, n_local, PAD)[..., :down_rows]
        g_up = g_up.transpose(1, 2, 3, 0, 4).reshape(layers, up_rows, ffn)
        shape = (micro, rows, hidden)
        return x_final.reshape(shape), d_cur.reshape(shape), g_up, jnp.stack(grads_down)

    spec = P(None, ALL_AXES, None)
    return jax.shard_map(body, mesh=mesh, in_specs=(spec,) * 4, out_specs=(spec,) * 4, check_vma=False)
```

```python
import functools
import math

import jax
import jax.numpy as jnp
from jax import lax
from jax.experimental import pallas as pl
from jax.experimental.pallas import tpu as pltpu
from jax.sharding import PartitionSpec as P

NORM_EPS = 1e-6
ALL_AXES = ("local", "data")
PAD = 48
RING = 4
CORES = 2
HALVES = (0, 1)
SLAB = 2**15
SLOTS = 101
WIDE = 1024
GRAD_SLOTS = 35
NORM_ROWS = 16
GELU_ROWS = 32
STEP = 512
VMEM = 62 * 2**20
ROWS = (((1,), (1,)), ((), ()))
MESH = pl.DeviceIdType.MESH


def norm_f32(x_f32):
    return x_f32 * lax.rsqrt(jnp.mean(x_f32 * x_f32, axis=-1, keepdims=True) + NORM_EPS)


def gelu_f32(pre_f32):
    return jax.nn.gelu(pre_f32, approximate=True)


class Place:
    def __init__(self):
        local, data = lax.axis_index("local"), lax.axis_index("data")
        self.z, self.y = local // RING, local % RING
        self.x, self.core = data // CORES, data % CORES

    def dev(self, **at):
        z, y, x, core = (at.get(name, getattr(self, name)) for name in ("z", "y", "x", "core"))
        return (z * RING + y, x * CORES + core)

    def along(self, axis):
        me = getattr(self, axis)
        left, right, _ = around(me)
        return me, self.dev(**{axis: right}), self.dev(**{axis: left})

    def turns(self, sign=1):
        return [(lax.rem(self.x + RING + sign * dx, RING), lax.rem(self.core + dc, CORES))
                for dx in range(RING) for dc in range(CORES)][1:]

    def sibling(self):
        return self.dev(core=1 - self.core)


def around(me):
    return [lax.rem(me + k, RING) for k in (3, 1, 2)]


def slab(i, n):
    return pl.ds(pl.multiple_of(i * n, n), n)


def greet(devices, meanwhile=None):
    barrier = pltpu.get_barrier_semaphore()
    for device in devices:
        pl.semaphore_signal(barrier, inc=1, device_id=device, device_id_type=MESH)
    if meanwhile is not None:
        meanwhile()
    pl.semaphore_wait(barrier, len(devices))


class Sender:
    def __init__(self, send_sems, recv_sems):
        self.send_sems, self.recv_sems, self.started = send_sems, recv_sems, []

    def copy(self, slot, src, dst, device, there=None):
        there = slot if there is None else there
        c = pltpu.make_async_remote_copy(src_ref=src, dst_ref=dst, send_sem=self.send_sems.at[slot],
                                         recv_sem=self.recv_sems.at[there], device_id=device, device_id_type=MESH)
        return c

    def start(self, slot, src, dst, device, there=None):
        c = self.copy(slot, src, dst, device, there)
        c.start()
        self.started.append(c)

    def arrived(self, slot, dst, device):
        self.copy(0, dst, dst, device, slot).wait_recv()

    def drain(self):
        for c in self.started:
            c.wait_send()


class RingGather:
    def __init__(self, sender, base, ring, own, block):
        self.s, self.base, self.own, self.block = sender, base, own, block
        self.me, self.right, self.left = ring
        self.prev, self.next, self.far = around(self.me)

    def start(self, halves=HALVES):
        for h in halves:
            self.s.start(self.base + h, self.own(h), self.block(self.me, h), self.right)
            self.s.start(self.base + 3 - h, self.own(1 - h), self.block(self.me, 1 - h), self.left)

    def relay(self):
        self.s.arrived(self.base, self.block(self.prev, 0), self.left)
        self.s.start(self.base + 4, self.block(self.prev, 0), self.block(self.prev, 0), self.right)
        self.s.arrived(self.base + 3, self.block(self.next, 1), self.right)
        self.s.start(self.base + 5, self.block(self.next, 1), self.block(self.next, 1), self.left)

    def near(self):
        self.s.arrived(self.base + 1, self.block(self.prev, 1), self.left)
        self.s.arrived(self.base + 2, self.block(self.next, 0), self.right)

    def finish(self):
        self.s.arrived(self.base + 4, self.block(self.far, 0), self.left)
        self.s.arrived(self.base + 5, self.block(self.far, 1), self.right)


class WeightGather:
    def __init__(self, p, sender, base, src, dst, cols=None):
        ring_y, ring_z = p.along("y"), p.along("z")
        start, cols = (0, src.shape[1]) if cols is None else cols
        rows = src.shape[0]
        if start == 0 and cols < WIDE:
            quarter = rows // 4
            sub = lambda part, h: (pl.ds((2 * part + h) * quarter, quarter), slice(None))
        else:
            quarter = cols // 4
            sub = lambda part, h: (slice(None), pl.ds(start + (2 * part + h) * quarter, quarter))
        block2 = (lambda i, h: dst.at[(i, slice(None)) + sub(0, h)], lambda i, h: dst.at[(slice(None), i) + sub(1, h)])
        self.block2 = block2
        self.stage1 = (RingGather(sender, base, ring_y, lambda h: src.at[sub(0, h)], lambda i, h: dst.at[(p.z, i) + sub(0, h)]),
                       RingGather(sender, base + 6, ring_z, lambda h: src.at[sub(1, h)], lambda i, h: dst.at[(i, p.y) + sub(1, h)]))
        self.stage2 = (RingGather(sender, base + 12, ring_z, lambda h: block2[0](p.z, h), block2[0]),
                       RingGather(sender, base + 18, ring_y, lambda h: block2[1](p.y, h), block2[1]))

    def start(self):
        for g in self.stage1:
            g.start()

    def second(self, keep=None):
        self.early()
        self.late(keep)

    def early(self):
        for g in self.stage1:
            g.relay()

    def late(self, keep=None):
        for g in self.stage1:
            g.near()
            g.finish()
        if keep is not None:
            keep.wait()
        for g in self.stage2:
            g.start()

    def relay(self):
        for g in self.stage2:
            g.relay()

    def finish(self):
        for g in self.stage2:
            g.near()
            g.finish()


class Exchange:
    SLOTS = 62

    def __init__(self, x_ref, xs, first, first_dst, second, second_dst, send_sems, recv_sems, keep_sem):
        p = Place()
        ring_x, ring_y, ring_z = p.along("x"), p.along("y"), p.along("z")
        self.p, self.sib, self.xs, self.x_ref = p, p.sibling(), xs, x_ref
        c = p.core
        self.keep = pltpu.make_async_copy(second, second_dst.at[p.z, p.y], keep_sem)
        self.keep.start()
        first_dst[p.z, p.y] = first[...]
        xs[p.x, c] = x_ref[...]
        greet([ring_x[1], ring_x[2], ring_y[1], ring_y[2], ring_z[1], ring_z[2], self.sib])
        self.s = Sender(send_sems, recv_sems)
        self.gx = RingGather(self.s, 0, ring_x, lambda h: x_ref.at[h], lambda i, h: xs.at[i, c, h])
        self.first = WeightGather(p, self.s, 14, first, first_dst)
        self.second = WeightGather(p, self.s, 38, second, second_dst)

    def give(self, k, i, h, src=None):
        at = self.xs.at[i, self.p.core, h]
        self.s.start(6 + k, at if src is None else src, at, self.sib)

    def take(self, k, i, h):
        self.s.arrived(6 + k, self.xs.at[i, 1 - self.p.core, h], self.sib)

    def run(self, early, compute):
        gx, me = self.gx, self.p.x
        self.first.start()
        gx.start()
        for h in HALVES:
            self.give(h, me, h, self.x_ref.at[h])
        self.second.start()
        self.first.second()
        self.second.early()
        for h in HALVES:
            self.take(h, me, h)
        early(me, True)
        gx.relay()
        self.give(2, gx.prev, 0)
        self.give(3, gx.next, 1)
        self.first.relay()
        self.second.late(self.keep)
        self.first.finish()
        compute(me, True)
        gx.near()
        self.give(4, gx.prev, 1)
        self.give(5, gx.next, 0)
        self.take(2, gx.prev, 0)
        self.take(4, gx.prev, 1)
        self.second.relay()
        early(gx.prev, False)
        compute(gx.prev, False)
        self.take(3, gx.next, 1)
        self.take(5, gx.next, 0)
        gx.finish()
        self.give(6, gx.far, 0)
        self.give(7, gx.far, 1)
        early(gx.next, False)
        compute(gx.next, False)
        self.take(6, gx.far, 0)
        self.take(7, gx.far, 1)
        early(gx.far, False, True)
        compute(gx.far, False)
        self.second.finish()
        self.s.drain()


def forward_kernel(first, tokens_ref, up_ref, down_ref, u_ref, slope_ref, act_ref, next_ref, *refs):
    if first:
        ups, *refs = refs
        up_src = ups.at[0]
    else:
        up_src = up_ref
    x_ref, y_ref, to_sib, from_sib, xs, w1, wide, shards, w2, acts, passing, send_sems, recv_sems, sems = refs
    p = Place()
    me, right, left = p.along("x")
    ring_y, ring_z = p.along("y"), p.along("z")
    c, o, sib = p.core, 1 - p.core, p.sibling()
    hidden, width = xs.shape[-1], w1.shape[-1]
    rows, half_cols = down_ref.shape[0], down_ref.shape[1] // 2
    own = y_ref.shape[0]
    half = own // 2
    mine = pl.ds(pl.multiple_of(me * rows, 16), rows)

    def prepare():
        shards[mine, :] = down_ref[...]
        for h in HALVES:
            @pl.loop(0, half // NORM_ROWS)
            def _(r):
                at = slab(r, NORM_ROWS)
                u = norm_f32(tokens_ref[h, at, :].astype(jnp.float32)).astype(jnp.bfloat16)
                x_ref[h, at, :] = u
                xs[me, c, h, at, :] = u

    prev, next_, far = around(me)
    over_data = [p.dev(x=x, core=core) for x, core in p.turns()] if first else [right, left, sib]
    greet(over_data + [ring_y[1], ring_y[2], ring_z[1], ring_z[2]], prepare)
    s = Sender(send_sems, recv_sems)
    gx = RingGather(s, 0, (me, right, left), lambda h: x_ref.at[h], lambda i, h: xs.at[i, c, h])
    gd = RingGather(s, 6, (me, right, left), lambda h: down_ref.at[:, pl.ds(h * half_cols, half_cols)],
                    lambda i, h: shards.at[pl.ds(pl.multiple_of(i * rows, 16), rows), pl.ds(h * half_cols, half_cols)])
    up = WeightGather(p, s, 12, up_src, w1)
    downs = [WeightGather(p, s, base, shards, w2, (k * WIDE, WIDE)) for k, base in enumerate((36, 75))]
    saves = []

    def give(k, i, h, src=None):
        at = xs.at[i, c, h]
        s.start(60 + k, at if src is None else src, at, sib)

    def take(k, i, h):
        s.arrived(60 + k, xs.at[i, o, h], sib)

    def save(src, dst):
        copy = pltpu.make_async_copy(src, dst, sems.at[len(saves)])
        copy.start()
        saves.append(copy)

    def compute(i):
        if saves:
            saves[-1].wait()
        save(xs.at[i], u_ref.at[i])
        wide[...] = jnp.dot(xs[i].reshape(wide.shape[0], hidden), w1[...].reshape(hidden, width),
                            preferred_element_type=jnp.float32)

        @pl.loop(0, wide.shape[0] // GELU_ROWS)
        def _(r):
            at = slab(r, GELU_ROWS)
            act, pull = jax.vjp(gelu_f32, wide[at, :].astype(jnp.bfloat16).astype(jnp.float32))
            act_ref[i, at, :] = act.astype(jnp.bfloat16)
            wide[at, :] = pull(jnp.ones_like(act))[0]

        save(wide, slope_ref.at[i])

    def own_rows():
        gx.start()
        for h in HALVES:
            give(h, me, h, x_ref.at[h])

    def down_rows():
        gd.near()
        gd.finish()
        w2[p.z, p.y] = shards[...]

    def near_rows():
        gx.relay()
        give(2, prev, 0)
        give(3, next_, 1)

    gd.start()
    if first:
        rank = me * CORES + c
        piece = up_ref.shape[2]
        for k, (x, core) in enumerate(p.turns()):
            s.start(SLOTS + k, up_ref.at[x * CORES + core], ups.at[:, slab(rank, piece)], p.dev(x=x, core=core))
        ups[:, slab(rank, piece), :] = up_ref[rank]
        gd.relay()
        own_rows()
        down_rows()
        for down in downs:
            down.start()
        for k, (x, core) in enumerate(p.turns(-1)):
            s.arrived(SLOTS + k, ups.at[:, slab(x * CORES + core, piece)], sib)
        up.start()
        w1[p.z, p.y] = up_src[...]
        for down in downs:
            down.early()
        up.second()
        near_rows()
        up.relay()
        downs[0].late()
    else:
        up.start()
        w1[p.z, p.y] = up_src[...]
        gd.relay()
        own_rows()
        up.second()
        down_rows()
        up.relay()
        for down in downs:
            down.start()
        near_rows()
    up.finish()
    take(0, me, 0)
    take(1, me, 1)
    compute(me)
    acts[me] = act_ref[me]
    if not first:
        for down in downs:
            down.early()
    gx.near()
    give(4, prev, 1)
    give(5, next_, 0)
    take(2, prev, 0)
    take(4, prev, 1)
    compute(prev)
    s.start(68, act_ref.at[prev], acts.at[me], left)
    if not first:
        downs[0].late()
    take(3, next_, 1)
    take(5, next_, 0)
    compute(next_)
    s.start(69, act_ref.at[next_], acts.at[me], right)
    gx.finish()
    give(6, far, 0)
    give(7, far, 1)
    take(6, far, 0)
    take(7, far, 1)
    compute(far)
    low, high = pl.ds(0, own), pl.ds(own, own)
    s.start(70, act_ref.at[far, low], passing.at[0], right)
    s.start(71, act_ref.at[far, high], passing.at[1], left)
    downs[0].relay()
    downs[1].late()
    s.arrived(70, passing.at[0], left)
    s.start(72, passing.at[0], acts.at[prev, low], right)
    s.arrived(71, passing.at[1], right)
    s.start(73, passing.at[1], acts.at[next_, high], left)
    downs[1].relay()
    s.arrived(68, acts.at[next_], right)
    s.arrived(69, acts.at[prev], left)
    s.arrived(72, acts.at[far, low], left)
    s.arrived(73, acts.at[far, high], right)

    def product(k, core, dst):
        @pl.loop(0, WIDE // STEP)
        def _(n):
            at = slab(k * (WIDE // STEP) + n, STEP)
            total = None
            for x in range(RING):
                w = w2.at[:, :, pl.ds(x * rows, rows), at][...].reshape(width, STEP)
                term = jnp.dot(acts[x, slab(core, own), :], w, preferred_element_type=jnp.float32)
                total = term if total is None else total + term
            dst[:, at] = total

    for k, down in enumerate(downs):
        down.finish()
        product(k, o, to_sib)
        at = pl.ds(k * WIDE, WIDE)
        s.start(SLOTS - 1 - k, to_sib.at[:, at], from_sib.at[:, at], sib)
        product(k, c, y_ref)
    for k in HALVES:
        at = pl.ds(k * WIDE, WIDE)
        s.arrived(SLOTS - 1 - k, from_sib.at[:, at], sib)
    for h in HALVES:
        @pl.loop(0, half // NORM_ROWS)
        def _(r):
            at = slab(r, NORM_ROWS)
            there = pl.ds(pl.multiple_of(h * half + r * NORM_ROWS, NORM_ROWS), NORM_ROWS)
            y = y_ref[there, :] + from_sib[there, :]
            next_ref[h, at, :] = (tokens_ref[h, at, :].astype(jnp.float32) + y).astype(jnp.bfloat16)

    for copy in saves[::2] + saves[-1:]:
        copy.wait()
    s.drain()


def forward(x, up, down, first):
    vmem, anywhere = pl.BlockSpec(memory_space=pltpu.VMEM), pl.BlockSpec(memory_space=pl.ANY)
    micro, rows, hidden = x.shape
    own, width = micro * rows, up.shape[-1]
    block = CORES * own
    bf16, f32, dma = jnp.bfloat16, jnp.float32, pltpu.SemaphoreType.DMA
    shards = (RING * down.shape[0], hidden)
    n_data = RING * CORES
    up_shape = (n_data * up.shape[2], width) if first else up.shape
    outs = [jax.ShapeDtypeStruct((RING, CORES) + x.shape, bf16), jax.ShapeDtypeStruct((RING, block, width), f32),
            jax.ShapeDtypeStruct((RING, block, width), bf16), jax.ShapeDtypeStruct(x.shape, bf16)]
    if first:
        outs.append(jax.ShapeDtypeStruct((up.shape[1],) + up_shape, bf16))
    slots = SLOTS + n_data
    return pl.pallas_call(
        functools.partial(forward_kernel, first),
        out_shape=outs,
        in_specs=[vmem] * 3,
        out_specs=[anywhere] * 2 + [vmem] * (len(outs) - 2),
        scratch_shapes=[pltpu.VMEM(x.shape, bf16), *[pltpu.VMEM((own, hidden), f32)] * 3,
                        pltpu.VMEM((RING, CORES) + x.shape, bf16), pltpu.VMEM((RING, RING) + up_shape, bf16),
                        pltpu.VMEM((block, width), f32), pltpu.VMEM(shards, bf16),
                        pltpu.VMEM((RING, RING) + shards, bf16), pltpu.VMEM((RING, block, width), bf16),
                        pltpu.VMEM((2, own, width), bf16), dma((slots,)), dma((slots,)), dma((8,))],
        compiler_params=pltpu.CompilerParams(collective_id=4 if first else 0, has_side_effects=True, vmem_limit_bytes=VMEM),
        name="forward",
    )(x, up, down)


def back_kernel(x_ref, up_ref, down_ref, u_hbm, slope_hbm, act_hbm, z_ref, w1_ref, g_up, g_down,
                xs, w2, wide, us, slopes, acts, acc_up, acc_down, flipped, send_sems, recv_sems, sems):
    loads = [pltpu.make_async_copy(src, dst, sems.at[1 + k])
             for k, (src, dst) in enumerate(((slope_hbm, slopes), (act_hbm, acts), (u_hbm, us)))]
    for load in loads:
        load.start()
    hidden, width = xs.shape[-1], z_ref.shape[-1]
    block = wide.shape[0]
    ex = Exchange(x_ref, xs, down_ref, w2, up_ref, w1_ref, send_sems, recv_sems, sems.at[0])
    def accumulate(acc, left, right, i, initial):
        flipped[...] = left[i].T

        @pl.loop(0, hidden // STEP)
        def _(n):
            at = slab(n, STEP)
            term = jnp.dot(flipped[...], right.at[i, :, :, :, at][...].reshape(block, STEP), preferred_element_type=jnp.float32)
            if initial:
                acc[:, at] = term
            else:
                acc[:, at] += term

    cols, rows = g_up.shape[3], g_down.shape[2]
    copies = []

    def store(acc_at, grad, base):
        for k in range(RING * RING):
            copy = pltpu.make_async_copy(acc_at(k), grad.at[k // RING, k % RING], sems.at[base + k])
            copy.start()
            copies.append(copy)

    def early(i, initial, last=False):
        if initial:
            for load in loads:
                load.wait()
        accumulate(acc_down, acts, xs, i, initial)
        if last:
            store(lambda k: acc_down.at[pl.ds(k * rows, rows)], g_down, 4)

    def compute(i, initial):
        wide[...] = lax.dot_general(xs[i].reshape(block, hidden), w2[...].reshape(width, hidden), ROWS,
                                    preferred_element_type=jnp.float32)

        @pl.loop(0, block // GELU_ROWS)
        def _(r):
            at = slab(r, GELU_ROWS)
            z_ref[i, at, :] = (wide[at, :] * slopes[i, at, :]).astype(jnp.bfloat16)

        accumulate(acc_up, z_ref, us, i, initial)

    ex.run(early, compute)
    store(lambda k: acc_up.at[:, pl.ds(k * cols, cols)], g_up, 20)
    for copy in copies:
        copy.wait()


def gather_back(x, up, down, u_all, slope, act):
    vmem, anywhere = pl.BlockSpec(memory_space=pltpu.VMEM), pl.BlockSpec(memory_space=pl.ANY)
    hidden, width = x.shape[-1], up.shape[1]
    bf16, f32, dma = jnp.bfloat16, jnp.float32, pltpu.SemaphoreType.DMA
    return pl.pallas_call(
        back_kernel,
        out_shape=[jax.ShapeDtypeStruct(act.shape, bf16),
                   jax.ShapeDtypeStruct((RING, RING) + up.shape, bf16),
                   jax.ShapeDtypeStruct((RING, RING, width, hidden // (RING * RING)), f32),
                   jax.ShapeDtypeStruct((RING, RING) + down.shape, f32)],
        in_specs=[vmem] * 3 + [anywhere] * 3,
        out_specs=[vmem] + [anywhere] * 3,
        scratch_shapes=[pltpu.VMEM((RING, CORES) + x.shape, bf16), pltpu.VMEM((RING, RING) + down.shape, bf16),
                        pltpu.VMEM(slope.shape[1:], f32), pltpu.VMEM(u_all.shape, bf16), pltpu.VMEM(slope.shape, f32),
                        pltpu.VMEM(act.shape, bf16), pltpu.VMEM((width, hidden), f32), pltpu.VMEM((width, hidden), f32),
                        pltpu.VMEM(act.shape[:0:-1], bf16),
                        dma((Exchange.SLOTS,)), dma((Exchange.SLOTS,)), dma((36,))],
        compiler_params=pltpu.CompilerParams(collective_id=3, has_side_effects=True, vmem_limit_bytes=VMEM),
        name="gather_back",
    )(x, up, down, u_all, slope, act)


def add_into(dst, *terms):
    if len(dst.shape) > 2:
        for i in range(dst.shape[0]):
            add_into(dst.at[i], *(term.at[i] for term in terms))
        return

    rows = math.gcd(dst.shape[0], max(8, SLAB // dst.shape[1]))

    @pl.loop(0, dst.shape[0] // rows)
    def _(i):
        at = slab(i, rows)
        total = dst[at, :]
        for term in terms:
            total = total + term[at, :]
        dst[at, :] = total


class RingScatter:
    def __init__(self, sender, base, ring, block, relayed, arriving):
        self.s, self.base, self.block, self.relayed, self.arriving = sender, base, block, relayed, arriving
        self.me, self.right, self.left = ring
        self.prev, self.next, self.far = around(self.me)

    def start(self):
        self.s.start(self.base, self.block(self.far, 0), self.relayed(0), self.right)
        self.s.start(self.base + 1, self.block(self.far, 1), self.relayed(1), self.left)
        self.s.start(self.base + 2, self.block(self.next, 1), self.arriving(0, 1), self.right)
        self.s.start(self.base + 3, self.block(self.prev, 0), self.arriving(1, 0), self.left)

    def relay(self, to_next, to_prev):
        self.s.arrived(self.base, self.relayed(0), self.left)
        add_into(self.relayed(0), to_next)
        self.s.start(self.base + 4, self.relayed(0), self.arriving(0, 0), self.right)
        self.s.arrived(self.base + 1, self.relayed(1), self.right)
        add_into(self.relayed(1), to_prev)
        self.s.start(self.base + 5, self.relayed(1), self.arriving(1, 1), self.left)

    def finish(self):
        self.s.arrived(self.base + 2, self.arriving(0, 1), self.left)
        self.s.arrived(self.base + 3, self.arriving(1, 0), self.right)
        self.s.arrived(self.base + 4, self.arriving(0, 0), self.left)
        self.s.arrived(self.base + 5, self.arriving(1, 1), self.right)


class GradScatter:
    def __init__(self, p, sender, base, up, down, bufs, sems):
        self.p, self.sems, self.up, self.down = p, sems, up, down
        (self.u_rel, self.u_arr, self.u_loc, self.u_own, self.u_rel2, self.u_arr2,
         self.d_rel, self.d_arr, self.d_loc, self.d_own, self.d_rel2, self.d_arr2) = bufs
        ring_y, ring_z = p.along("y"), p.along("z")
        half = lambda h: pl.ds(2 * h, 2)
        u_rows, d_rows = up.shape[2] // 2, down.shape[2] // 2
        u_part, d_part = (lambda h: pl.ds(h * u_rows, u_rows)), (lambda h: pl.ds(h * d_rows, d_rows))
        self.up1 = RingScatter(sender, base, ring_y, lambda i, h: up.at[half(h), i], lambda h: self.u_rel.at[h],
                               lambda side, h: self.u_arr.at[side, half(h)])
        self.down1 = RingScatter(sender, base + 6, ring_z, lambda i, h: down.at[i, half(h)], lambda h: self.d_rel.at[h],
                                 lambda side, h: self.d_arr.at[side, half(h)])
        self.up2 = RingScatter(sender, base + 12, ring_z, lambda i, h: self.u_own.at[i, u_part(h)], lambda h: self.u_rel2.at[h],
                               lambda side, h: self.u_arr2.at[side, u_part(h)])
        self.down2 = RingScatter(sender, base + 18, ring_y, lambda i, h: self.d_own.at[i, d_part(h)], lambda h: self.d_rel2.at[h],
                                 lambda side, h: self.d_arr2.at[side, d_part(h)])
        self.u_part, self.d_part = u_part, d_part
        u, d = self.up1, self.down1
        pairs = [(up.at[half(0), u.next], self.u_loc.at[0]), (up.at[half(1), u.prev], self.u_loc.at[1]),
                 (up.at[:, u.me], self.u_own), (down.at[d.next, half(0)], self.d_loc.at[0]),
                 (down.at[d.prev, half(1)], self.d_loc.at[1]), (down.at[d.me], self.d_own)]
        self.loads = [pltpu.make_async_copy(src, dst, sems.at[k]) for k, (src, dst) in enumerate(pairs)]

    def load(self):
        for copy in self.loads:
            copy.start()

    def start(self):
        self.up1.start()
        self.down1.start()

    def relay(self):
        for copy in self.loads:
            copy.wait()
        self.up1.relay(self.u_loc.at[0], self.u_loc.at[1])
        self.down1.relay(self.d_loc.at[0], self.d_loc.at[1])

    def second(self):
        self.up1.finish()
        add_into(self.u_own, self.u_arr.at[0], self.u_arr.at[1])
        self.up2.start()
        self.down1.finish()
        add_into(self.d_own, self.d_arr.at[0], self.d_arr.at[1])
        self.down2.start()
        u, d = self.up2, self.down2
        u.relay(self.u_own.at[u.next, self.u_part(0)], self.u_own.at[u.prev, self.u_part(1)])
        d.relay(self.d_own.at[d.next, self.d_part(0)], self.d_own.at[d.prev, self.d_part(1)])

    def finish(self, up_out, down_out):
        self.up2.finish()
        self.down2.finish()
        up_out[...] = (self.u_own[self.up2.me] + self.u_arr2[0] + self.u_arr2[1]).T
        down_out[...] = self.d_own[self.down2.me] + self.d_arr2[0] + self.d_arr2[1]

    @staticmethod
    def buffers(up, down):
        f32 = jnp.float32
        out = []
        for rows, cols in (up.shape[2:], down.shape[2:]):
            out += [(2, 2, rows, cols), (2, RING, rows, cols), (2, 2, rows, cols), (RING, rows, cols),
                    (2, rows // 2, cols), (2, rows, cols)]
        return [pltpu.VMEM(shape, f32) for shape in out]


def scatter_kernel(h_ref, w_ref, *refs):
    p = Place()
    me, right, left = p.along("x")
    sib, c, o = p.sibling(), p.core, 1 - p.core
    (g_up, g_down, x_ref, c_ref, dx_ref, up_out, down_out, y_ref, to_sib, from_sib, acc, relayed, arriving, send_sems, recv_sems,
     up_sum, local_sems, *bufs) = refs
    ring_y, ring_z = p.along("y"), p.along("z")
    turns = p.turns()
    greet([p.dev(x=x, core=core) for x, core in turns] + [ring_y[1], ring_y[2], ring_z[1], ring_z[2]])
    s = Sender(send_sems, recv_sems)
    grads = GradScatter(p, s, 10, g_up, g_down, bufs, local_sems)
    grads.start()
    grads.load()
    hidden = y_ref.shape[1]
    rows = y_ref.shape[0] // 2
    first, second = pl.ds(0, rows), pl.ds(rows, rows)

    def product(dx, core, dst, part=slice(None)):
        block = lax.rem(me + dx, RING)

        @pl.loop(0, hidden // STEP)
        def _(n):
            at = slab(n, STEP)
            dst[:, at] = lax.dot_general(h_ref[block, core, part, :], w_ref[at, :], ROWS,
                                         preferred_element_type=jnp.float32)

    def both(k, dx, dst):
        product(dx, o, to_sib.at[k])
        s.start(k, to_sib.at[k], from_sib.at[k], sib)
        product(dx, c, dst)

    def joined(k, dst):
        s.arrived(k, from_sib.at[k], sib)
        add_into(dst, from_sib.at[k])

    parts = ((first, right, 0), (second, left, GRAD_SLOTS - 1))
    for h, (part, _, slot) in enumerate(parts):
        product(2, o, to_sib.at[0, part], part)
        s.start(slot, to_sib.at[0, part], from_sib.at[0, part], sib)
    for h, (part, to, slot) in enumerate(parts):
        product(2, c, acc.at[0, part], part)
        s.arrived(slot, from_sib.at[0, part], sib)
        add_into(acc.at[0, part], from_sib.at[0, part])
        s.start(4 + h, acc.at[0, part], relayed.at[h], to)
    both(1, 1, acc.at[1])
    both(2, 3, acc.at[2])
    joined(1, acc.at[1])
    s.start(6, acc.at[1, second], arriving.at[0, second], right)
    joined(2, acc.at[2])
    s.start(7, acc.at[2, first], arriving.at[1, first], left)
    both(3, 0, y_ref)
    joined(3, y_ref)
    grads.relay()
    s.arrived(4, relayed.at[0], left)
    add_into(acc.at[1, first], relayed.at[0])
    s.start(8, acc.at[1, first], arriving.at[0, first], right)
    s.arrived(5, relayed.at[1], right)
    add_into(acc.at[2, second], relayed.at[1])
    s.start(9, acc.at[2, second], arriving.at[1, second], left)
    grads.second()
    grads.finish(up_sum, down_out)
    mine = me * CORES + c
    piece = up_out.shape[1]
    keep = pltpu.make_async_copy(up_sum.at[slab(mine, piece)], up_out.at[mine], local_sems.at[6])
    keep.start()
    for k, (x, core) in enumerate(turns):
        to = x * CORES + core
        s.start(GRAD_SLOTS + k, up_sum.at[slab(to, piece)], up_out.at[mine], p.dev(x=x, core=core))
    s.arrived(6, arriving.at[0, second], left)
    s.arrived(7, arriving.at[1, first], right)
    s.arrived(8, arriving.at[0, first], left)
    s.arrived(9, arriving.at[1, second], right)
    for h in HALVES:
        @pl.loop(0, rows // NORM_ROWS)
        def _(r):
            at = slab(r, NORM_ROWS)
            there = pl.ds(pl.multiple_of(h * rows + r * NORM_ROWS, NORM_ROWS), NORM_ROWS)
            v = y_ref[there, :] + arriving[0, there, :] + arriving[1, there, :]
            pull = jax.vjp(norm_f32, x_ref[h, at, :].astype(jnp.float32))[1]
            dx_ref[h, at, :] = (c_ref[h, at, :].astype(jnp.float32) + pull(v)[0]).astype(jnp.bfloat16)

    for k, (x, core) in enumerate(p.turns(-1)):
        s.arrived(GRAD_SLOTS + k, up_out.at[x * CORES + core], p.dev(x=x, core=core))
    keep.wait()
    s.drain()


def scatter(h, w, grads, x, c):
    rows, width = h.shape[2:]
    hidden = w.shape[0]
    vmem, anywhere = pl.BlockSpec(memory_space=pltpu.VMEM), pl.BlockSpec(memory_space=pl.ANY)
    f32 = jnp.float32
    up_rows, down_rows = grads[0].shape[3], grads[1].shape[2]
    n_data = RING * CORES
    slots = GRAD_SLOTS + n_data
    return pl.pallas_call(
        scatter_kernel,
        out_shape=[jax.ShapeDtypeStruct(x.shape, x.dtype),
                   jax.ShapeDtypeStruct((n_data, up_rows // n_data, width), f32), jax.ShapeDtypeStruct((down_rows, hidden), f32)],
        in_specs=[vmem] * 2 + [anywhere] * 2 + [vmem] * 2,
        out_specs=[vmem] * 3,
        scratch_shapes=[pltpu.VMEM((rows, hidden), f32), pltpu.VMEM((RING, rows, hidden), f32), pltpu.VMEM((RING, rows, hidden), f32),
                        pltpu.VMEM((3, rows, hidden), f32), pltpu.VMEM((2, rows // 2, hidden), f32),
                        pltpu.VMEM((2, rows, hidden), f32),
                        pltpu.SemaphoreType.DMA((slots,)), pltpu.SemaphoreType.DMA((slots,)),
                        pltpu.VMEM((up_rows, width), f32), pltpu.SemaphoreType.DMA((7,))] + GradScatter.buffers(*grads),
        compiler_params=pltpu.CompilerParams(collective_id=2, has_side_effects=True, vmem_limit_bytes=VMEM),
        name="scatter_grads",
    )(h, w, *grads, x, c)


def solution(mesh):
    n_data = mesh.shape["data"]
    n_local = mesh.shape["local"]

    def body(tokens, cotangent, w_up, w_down):
        micro, rows, hidden = tokens.shape
        layers, up_rows, ffn = w_up.shape
        down_rows = w_down.shape[1]
        pad = PAD - down_rows
        width = n_local * PAD
        own = micro * rows

        up = w_up.reshape(layers, up_rows, n_local, n_data, down_rows)
        up = jnp.pad(up, ((0, 0),) * 4 + ((0, pad),))
        up = up.transpose(3, 0, 1, 2, 4).reshape(n_data, layers, up_rows, width)
        down = jnp.pad(w_down, ((0, 0), (0, pad), (0, 0)))

        def blocks(h):
            return h.reshape(RING, CORES, own, width)

        x_cur = tokens
        saved = []
        for layer in range(layers):
            u_all, slope, act, x_next, *ups = forward(x_cur, up if layer == 0 else up[layer], down[layer], layer == 0)
            if ups:
                up, = ups
            saved.append((x_cur, u_all, slope, act))
            x_cur = x_next
        x_final = x_cur

        d_cur, x_final = lax.optimization_barrier((cotangent, x_final))
        grads_up = [None] * layers
        grads_down = [None] * layers
        for layer in reversed(range(layers)):
            x_in, u_all, slope, act = saved[layer]
            z, w1, g_up, g_down = gather_back(d_cur, up[layer], down[layer], u_all, slope, act)
            d_cur, grads_up[layer], g_down = scatter(blocks(z), w1.reshape(hidden, width), (g_up, g_down), x_in, d_cur)
            grads_down[layer] = g_down[:down_rows]
        g_up = jnp.stack(grads_up, 1).reshape(n_data, layers, up_rows, n_local, PAD)[..., :down_rows]
        g_up = g_up.transpose(1, 2, 3, 0, 4).reshape(layers, up_rows, ffn)
        return x_final, d_cur, g_up, jnp.stack(grads_down)

    spec = P(None, ALL_AXES, None)
    return jax.shard_map(body, mesh=mesh, in_specs=(spec,) * 4, out_specs=(spec,) * 4, check_vma=False)
```

```python
import functools
import math

import jax
import jax.numpy as jnp
from jax import lax
from jax.experimental import pallas as pl
from jax.experimental.pallas import tpu as pltpu
from jax.sharding import PartitionSpec as P

NORM_EPS = 1e-6
ALL_AXES = ("local", "data")
PAD = 48
RING = 4
CORES = 2
HALVES = (0, 1)
SLAB = 2**15
SLOTS = 101
WIDE = 1024
GRAD_SLOTS = 35
NORM_ROWS = 16
GELU_ROWS = 32
STEP = 512
TILE = 256
VMEM = 62 * 2**20
ROWS = (((1,), (1,)), ((), ()))
MESH = pl.DeviceIdType.MESH


def norm_f32(x_f32):
    return x_f32 * lax.rsqrt(jnp.mean(x_f32 * x_f32, axis=-1, keepdims=True) + NORM_EPS)


def gelu_f32(pre_f32):
    return jax.nn.gelu(pre_f32, approximate=True)


class Place:
    def __init__(self):
        local, data = lax.axis_index("local"), lax.axis_index("data")
        self.z, self.y = local // RING, local % RING
        self.x, self.core = data // CORES, data % CORES

    def dev(self, **at):
        z, y, x, core = (at.get(name, getattr(self, name)) for name in ("z", "y", "x", "core"))
        return (z * RING + y, x * CORES + core)

    def along(self, axis):
        me = getattr(self, axis)
        left, right, _ = around(me)
        return me, self.dev(**{axis: right}), self.dev(**{axis: left})

    def turns(self, sign=1):
        return [(lax.rem(self.x + RING + sign * dx, RING), lax.rem(self.core + dc, CORES))
                for dx in range(RING) for dc in range(CORES)][1:]

    def sibling(self):
        return self.dev(core=1 - self.core)


def around(me):
    return [lax.rem(me + k, RING) for k in (3, 1, 2)]


def slab(i, n):
    return pl.ds(pl.multiple_of(i * n, n), n)


def greet(devices, meanwhile=None):
    barrier = pltpu.get_barrier_semaphore()
    for device in devices:
        pl.semaphore_signal(barrier, inc=1, device_id=device, device_id_type=MESH)
    if meanwhile is not None:
        meanwhile()
    pl.semaphore_wait(barrier, len(devices))


class Sender:
    def __init__(self, send_sems, recv_sems):
        self.send_sems, self.recv_sems, self.started = send_sems, recv_sems, []

    def copy(self, slot, src, dst, device, there=None):
        there = slot if there is None else there
        c = pltpu.make_async_remote_copy(src_ref=src, dst_ref=dst, send_sem=self.send_sems.at[slot],
                                         recv_sem=self.recv_sems.at[there], device_id=device, device_id_type=MESH)
        return c

    def start(self, slot, src, dst, device, there=None):
        c = self.copy(slot, src, dst, device, there)
        c.start()
        self.started.append(c)

    def arrived(self, slot, dst, device):
        self.copy(0, dst, dst, device, slot).wait_recv()

    def drain(self):
        for c in self.started:
            c.wait_send()


class RingGather:
    def __init__(self, sender, base, ring, own, block):
        self.s, self.base, self.own, self.block = sender, base, own, block
        self.me, self.right, self.left = ring
        self.prev, self.next, self.far = around(self.me)

    def start(self, halves=HALVES):
        for h in halves:
            self.s.start(self.base + h, self.own(h), self.block(self.me, h), self.right)
            self.s.start(self.base + 3 - h, self.own(1 - h), self.block(self.me, 1 - h), self.left)

    def relay(self):
        self.s.arrived(self.base, self.block(self.prev, 0), self.left)
        self.s.start(self.base + 4, self.block(self.prev, 0), self.block(self.prev, 0), self.right)
        self.s.arrived(self.base + 3, self.block(self.next, 1), self.right)
        self.s.start(self.base + 5, self.block(self.next, 1), self.block(self.next, 1), self.left)

    def near(self):
        self.s.arrived(self.base + 1, self.block(self.prev, 1), self.left)
        self.s.arrived(self.base + 2, self.block(self.next, 0), self.right)

    def finish(self):
        self.s.arrived(self.base + 4, self.block(self.far, 0), self.left)
        self.s.arrived(self.base + 5, self.block(self.far, 1), self.right)


class WeightGather:
    def __init__(self, p, sender, base, src, dst, cols=None):
        ring_y, ring_z = p.along("y"), p.along("z")
        start, cols = (0, src.shape[1]) if cols is None else cols
        rows = src.shape[0]
        if start == 0 and cols < WIDE:
            quarter = rows // 4
            sub = lambda part, h: (pl.ds((2 * part + h) * quarter, quarter), slice(None))
        else:
            quarter = cols // 4
            sub = lambda part, h: (slice(None), pl.ds(start + (2 * part + h) * quarter, quarter))
        block2 = (lambda i, h: dst.at[(i, slice(None)) + sub(0, h)], lambda i, h: dst.at[(slice(None), i) + sub(1, h)])
        self.block2 = block2
        self.stage1 = (RingGather(sender, base, ring_y, lambda h: src.at[sub(0, h)], lambda i, h: dst.at[(p.z, i) + sub(0, h)]),
                       RingGather(sender, base + 6, ring_z, lambda h: src.at[sub(1, h)], lambda i, h: dst.at[(i, p.y) + sub(1, h)]))
        self.stage2 = (RingGather(sender, base + 12, ring_z, lambda h: block2[0](p.z, h), block2[0]),
                       RingGather(sender, base + 18, ring_y, lambda h: block2[1](p.y, h), block2[1]))

    def start(self):
        for g in self.stage1:
            g.start()

    def second(self, keep=None):
        self.early()
        self.late(keep)

    def early(self):
        for g in self.stage1:
            g.relay()

    def late(self, keep=None):
        for g in self.stage1:
            g.near()
            g.finish()
        if keep is not None:
            keep.wait()
        for g in self.stage2:
            g.start()

    def relay(self):
        for g in self.stage2:
            g.relay()

    def finish(self):
        for g in self.stage2:
            g.near()
            g.finish()


class Exchange:
    SLOTS = 62

    def __init__(self, x_ref, xs, first, first_dst, second, second_dst, send_sems, recv_sems, keep_sem):
        p = Place()
        ring_x, ring_y, ring_z = p.along("x"), p.along("y"), p.along("z")
        self.p, self.sib, self.xs, self.x_ref = p, p.sibling(), xs, x_ref
        c = p.core
        self.keep = pltpu.make_async_copy(second, second_dst.at[p.z, p.y], keep_sem)
        self.keep.start()
        first_dst[p.z, p.y] = first[...]
        xs[p.x, c] = x_ref[...]
        greet([ring_x[1], ring_x[2], ring_y[1], ring_y[2], ring_z[1], ring_z[2], self.sib])
        self.s = Sender(send_sems, recv_sems)
        self.gx = RingGather(self.s, 0, ring_x, lambda h: x_ref.at[h], lambda i, h: xs.at[i, c, h])
        self.first = WeightGather(p, self.s, 14, first, first_dst)
        self.second = WeightGather(p, self.s, 38, second, second_dst)

    def give(self, k, i, h, src=None):
        at = self.xs.at[i, self.p.core, h]
        self.s.start(6 + k, at if src is None else src, at, self.sib)

    def take(self, k, i, h):
        self.s.arrived(6 + k, self.xs.at[i, 1 - self.p.core, h], self.sib)

    def run(self, early, compute):
        gx, me = self.gx, self.p.x
        self.first.start()
        gx.start()
        for h in HALVES:
            self.give(h, me, h, self.x_ref.at[h])
        self.second.start()
        self.first.second()
        self.second.early()
        for h in HALVES:
            self.take(h, me, h)
        early(me, True)
        gx.relay()
        self.give(2, gx.prev, 0)
        self.give(3, gx.next, 1)
        self.first.relay()
        self.second.late(self.keep)
        self.first.finish()
        compute(me, True)
        gx.near()
        self.give(4, gx.prev, 1)
        self.give(5, gx.next, 0)
        self.take(2, gx.prev, 0)
        self.take(4, gx.prev, 1)
        self.second.relay()
        early(gx.prev, False)
        compute(gx.prev, False)
        self.take(3, gx.next, 1)
        self.take(5, gx.next, 0)
        gx.finish()
        self.give(6, gx.far, 0)
        self.give(7, gx.far, 1)
        early(gx.next, False)
        compute(gx.next, False)
        self.take(6, gx.far, 0)
        self.take(7, gx.far, 1)
        early(gx.far, False, True)
        compute(gx.far, False)
        self.second.finish()
        self.s.drain()


def forward_kernel(first, tokens_ref, up_ref, down_ref, u_ref, slope_ref, act_ref, next_ref, *refs):
    if first:
        ups, *refs = refs
        up_src = ups.at[0]
    else:
        up_src = up_ref
    x_ref, y_ref, to_sib, from_sib, xs, w1, wide, shards, w2, acts, passing, send_sems, recv_sems, sems = refs
    p = Place()
    me, right, left = p.along("x")
    ring_y, ring_z = p.along("y"), p.along("z")
    c, o, sib = p.core, 1 - p.core, p.sibling()
    hidden, width = xs.shape[-1], w1.shape[-1]
    rows, half_cols = down_ref.shape[0], down_ref.shape[1] // 2
    own = y_ref.shape[0]
    half = own // 2
    mine = pl.ds(pl.multiple_of(me * rows, 16), rows)

    def prepare():
        shards[mine, :] = down_ref[...]
        for h in HALVES:
            @pl.loop(0, half // NORM_ROWS)
            def _(r):
                at = slab(r, NORM_ROWS)
                u = norm_f32(tokens_ref[h, at, :].astype(jnp.float32)).astype(jnp.bfloat16)
                x_ref[h, at, :] = u
                xs[me, c, h, at, :] = u

    prev, next_, far = around(me)
    over_data = [p.dev(x=x, core=core) for x, core in p.turns()] if first else [right, left, sib]
    greet(over_data + [ring_y[1], ring_y[2], ring_z[1], ring_z[2]], prepare)
    s = Sender(send_sems, recv_sems)
    gx = RingGather(s, 0, (me, right, left), lambda h: x_ref.at[h], lambda i, h: xs.at[i, c, h])
    gd = RingGather(s, 6, (me, right, left), lambda h: down_ref.at[:, pl.ds(h * half_cols, half_cols)],
                    lambda i, h: shards.at[pl.ds(pl.multiple_of(i * rows, 16), rows), pl.ds(h * half_cols, half_cols)])
    up = WeightGather(p, s, 12, up_src, w1)
    downs = [WeightGather(p, s, base, shards, w2, (k * WIDE, WIDE)) for k, base in enumerate((36, 75))]
    saves = []

    def give(k, i, h, src=None):
        at = xs.at[i, c, h]
        s.start(60 + k, at if src is None else src, at, sib)

    def take(k, i, h):
        s.arrived(60 + k, xs.at[i, o, h], sib)

    def save(src, dst):
        copy = pltpu.make_async_copy(src, dst, sems.at[len(saves)])
        copy.start()
        saves.append(copy)

    def compute(i):
        if saves:
            saves[-1].wait()
        save(xs.at[i], u_ref.at[i])

        @pl.loop(0, width // TILE)
        def _(n):
            at = slab(n, TILE)
            wide[:, at] = jnp.dot(xs[i].reshape(wide.shape[0], hidden), w1.at[:, :, :, at][...].reshape(hidden, TILE),
                                  preferred_element_type=jnp.float32)

        @pl.loop(0, wide.shape[0] // GELU_ROWS)
        def _(r):
            at = slab(r, GELU_ROWS)
            act, pull = jax.vjp(gelu_f32, wide[at, :].astype(jnp.bfloat16).astype(jnp.float32))
            act_ref[i, at, :] = act.astype(jnp.bfloat16)
            wide[at, :] = pull(jnp.ones_like(act))[0]

        save(wide, slope_ref.at[i])

    def own_rows():
        gx.start()
        for h in HALVES:
            give(h, me, h, x_ref.at[h])

    def down_rows():
        gd.near()
        gd.finish()
        w2[p.z, p.y] = shards[...]

    def near_rows():
        gx.relay()
        give(2, prev, 0)
        give(3, next_, 1)

    if first:
        rank = me * CORES + c
        piece = up_ref.shape[2]
        for k, (x, core) in enumerate(p.turns()):
            s.start(SLOTS + k, up_ref.at[x * CORES + core], ups.at[:, slab(rank, piece)], p.dev(x=x, core=core))
        ups[:, slab(rank, piece), :] = up_ref[rank]
    gd.start()
    if first:
        for k, (x, core) in enumerate(p.turns(-1)):
            s.arrived(SLOTS + k, ups.at[:, slab(x * CORES + core, piece)], sib)
    up.start()
    w1[p.z, p.y] = up_src[...]
    gd.relay()
    own_rows()
    up.second()
    down_rows()
    up.relay()
    for down in downs:
        down.start()
    near_rows()
    up.finish()
    take(0, me, 0)
    take(1, me, 1)
    compute(me)
    acts[me] = act_ref[me]
    for down in downs:
        down.early()
    gx.near()
    give(4, prev, 1)
    give(5, next_, 0)
    take(2, prev, 0)
    take(4, prev, 1)
    compute(prev)
    s.start(68, act_ref.at[prev], acts.at[me], left)
    downs[0].late()
    take(3, next_, 1)
    take(5, next_, 0)
    compute(next_)
    s.start(69, act_ref.at[next_], acts.at[me], right)
    gx.finish()
    give(6, far, 0)
    give(7, far, 1)
    take(6, far, 0)
    take(7, far, 1)
    compute(far)
    low, high = pl.ds(0, own), pl.ds(own, own)
    s.start(70, act_ref.at[far, low], passing.at[0], right)
    s.start(71, act_ref.at[far, high], passing.at[1], left)
    downs[0].relay()
    downs[1].late()
    s.arrived(70, passing.at[0], left)
    s.start(72, passing.at[0], acts.at[prev, low], right)
    s.arrived(71, passing.at[1], right)
    s.start(73, passing.at[1], acts.at[next_, high], left)
    downs[1].relay()
    s.arrived(68, acts.at[next_], right)
    s.arrived(69, acts.at[prev], left)
    s.arrived(72, acts.at[far, low], left)
    s.arrived(73, acts.at[far, high], right)

    def product(k, core, dst):
        @pl.loop(0, WIDE // TILE)
        def _(n):
            at = slab(k * (WIDE // TILE) + n, TILE)
            total = None
            for x in range(RING):
                w = w2.at[:, :, pl.ds(x * rows, rows), at][...].reshape(width, TILE)
                term = jnp.dot(acts[x, slab(core, own), :], w, preferred_element_type=jnp.float32)
                total = term if total is None else total + term
            dst[:, at] = total

    for k, down in enumerate(downs):
        down.finish()
        product(k, o, to_sib)
        at = pl.ds(k * WIDE, WIDE)
        s.start(SLOTS - 1 - k, to_sib.at[:, at], from_sib.at[:, at], sib)
        product(k, c, y_ref)
    for k in HALVES:
        at = pl.ds(k * WIDE, WIDE)
        s.arrived(SLOTS - 1 - k, from_sib.at[:, at], sib)
    for h in HALVES:
        @pl.loop(0, half // NORM_ROWS)
        def _(r):
            at = slab(r, NORM_ROWS)
            there = pl.ds(pl.multiple_of(h * half + r * NORM_ROWS, NORM_ROWS), NORM_ROWS)
            y = y_ref[there, :] + from_sib[there, :]
            next_ref[h, at, :] = (tokens_ref[h, at, :].astype(jnp.float32) + y).astype(jnp.bfloat16)

    for copy in saves[::2] + saves[-1:]:
        copy.wait()
    s.drain()


def forward(x, up, down, first):
    vmem, anywhere = pl.BlockSpec(memory_space=pltpu.VMEM), pl.BlockSpec(memory_space=pl.ANY)
    micro, rows, hidden = x.shape
    own, width = micro * rows, up.shape[-1]
    block = CORES * own
    bf16, f32, dma = jnp.bfloat16, jnp.float32, pltpu.SemaphoreType.DMA
    shards = (RING * down.shape[0], hidden)
    n_data = RING * CORES
    up_shape = (n_data * up.shape[2], width) if first else up.shape
    outs = [jax.ShapeDtypeStruct((RING, CORES) + x.shape, bf16), jax.ShapeDtypeStruct((RING, block, width), f32),
            jax.ShapeDtypeStruct((RING, block, width), bf16), jax.ShapeDtypeStruct(x.shape, bf16)]
    if first:
        outs.append(jax.ShapeDtypeStruct((up.shape[1],) + up_shape, bf16))
    slots = SLOTS + n_data
    return pl.pallas_call(
        functools.partial(forward_kernel, first),
        out_shape=outs,
        in_specs=[vmem] * 3,
        out_specs=[anywhere] * 2 + [vmem] * (len(outs) - 2),
        scratch_shapes=[pltpu.VMEM(x.shape, bf16), *[pltpu.VMEM((own, hidden), f32)] * 3,
                        pltpu.VMEM((RING, CORES) + x.shape, bf16), pltpu.VMEM((RING, RING) + up_shape, bf16),
                        pltpu.VMEM((block, width), f32), pltpu.VMEM(shards, bf16),
                        pltpu.VMEM((RING, RING) + shards, bf16), pltpu.VMEM((RING, block, width), bf16),
                        pltpu.VMEM((2, own, width), bf16), dma((slots,)), dma((slots,)), dma((8,))],
        compiler_params=pltpu.CompilerParams(collective_id=4 if first else 0, has_side_effects=True, vmem_limit_bytes=VMEM),
        name="forward",
    )(x, up, down)


def back_kernel(x_ref, up_ref, down_ref, u_hbm, slope_hbm, act_hbm, z_ref, w1_ref, g_up, g_down,
                xs, w2, wide, us, slopes, acts, acc_up, acc_down, flipped, send_sems, recv_sems, sems):
    loads = [pltpu.make_async_copy(src, dst, sems.at[1 + k])
             for k, (src, dst) in enumerate(((slope_hbm, slopes), (act_hbm, acts), (u_hbm, us)))]
    for load in loads:
        load.start()
    hidden, width = xs.shape[-1], z_ref.shape[-1]
    block = wide.shape[0]
    ex = Exchange(x_ref, xs, down_ref, w2, up_ref, w1_ref, send_sems, recv_sems, sems.at[0])
    def accumulate(acc, left, right, i, initial):
        flipped[...] = left[i].T

        @pl.loop(0, hidden // STEP)
        def _(n):
            at = slab(n, STEP)
            term = jnp.dot(flipped[...], right.at[i, :, :, :, at][...].reshape(block, STEP), preferred_element_type=jnp.float32)
            if initial:
                acc[:, at] = term
            else:
                acc[:, at] += term

    cols, rows = g_up.shape[3], g_down.shape[2]
    copies = []

    def store(acc_at, grad, base):
        for k in range(RING * RING):
            copy = pltpu.make_async_copy(acc_at(k), grad.at[k // RING, k % RING], sems.at[base + k])
            copy.start()
            copies.append(copy)

    def early(i, initial, last=False):
        if initial:
            for load in loads:
                load.wait()
        accumulate(acc_down, acts, xs, i, initial)
        if last:
            store(lambda k: acc_down.at[pl.ds(k * rows, rows)], g_down, 4)

    def compute(i, initial):
        wide[...] = lax.dot_general(xs[i].reshape(block, hidden), w2[...].reshape(width, hidden), ROWS,
                                    preferred_element_type=jnp.float32)

        @pl.loop(0, block // GELU_ROWS)
        def _(r):
            at = slab(r, GELU_ROWS)
            z_ref[i, at, :] = (wide[at, :] * slopes[i, at, :]).astype(jnp.bfloat16)

        accumulate(acc_up, z_ref, us, i, initial)

    ex.run(early, compute)
    store(lambda k: acc_up.at[:, pl.ds(k * cols, cols)], g_up, 20)
    for copy in copies:
        copy.wait()


def gather_back(x, up, down, u_all, slope, act):
    vmem, anywhere = pl.BlockSpec(memory_space=pltpu.VMEM), pl.BlockSpec(memory_space=pl.ANY)
    hidden, width = x.shape[-1], up.shape[1]
    bf16, f32, dma = jnp.bfloat16, jnp.float32, pltpu.SemaphoreType.DMA
    return pl.pallas_call(
        back_kernel,
        out_shape=[jax.ShapeDtypeStruct(act.shape, bf16),
                   jax.ShapeDtypeStruct((RING, RING) + up.shape, bf16),
                   jax.ShapeDtypeStruct((RING, RING, width, hidden // (RING * RING)), f32),
                   jax.ShapeDtypeStruct((RING, RING) + down.shape, f32)],
        in_specs=[vmem] * 3 + [anywhere] * 3,
        out_specs=[vmem] + [anywhere] * 3,
        scratch_shapes=[pltpu.VMEM((RING, CORES) + x.shape, bf16), pltpu.VMEM((RING, RING) + down.shape, bf16),
                        pltpu.VMEM(slope.shape[1:], f32), pltpu.VMEM(u_all.shape, bf16), pltpu.VMEM(slope.shape, f32),
                        pltpu.VMEM(act.shape, bf16), pltpu.VMEM((width, hidden), f32), pltpu.VMEM((width, hidden), f32),
                        pltpu.VMEM(act.shape[:0:-1], bf16),
                        dma((Exchange.SLOTS,)), dma((Exchange.SLOTS,)), dma((36,))],
        compiler_params=pltpu.CompilerParams(collective_id=3, has_side_effects=True, vmem_limit_bytes=VMEM),
        name="gather_back",
    )(x, up, down, u_all, slope, act)


def add_into(dst, *terms):
    if len(dst.shape) > 2:
        for i in range(dst.shape[0]):
            add_into(dst.at[i], *(term.at[i] for term in terms))
        return

    rows = math.gcd(dst.shape[0], max(8, SLAB // dst.shape[1]))

    @pl.loop(0, dst.shape[0] // rows)
    def _(i):
        at = slab(i, rows)
        total = dst[at, :]
        for term in terms:
            total = total + term[at, :]
        dst[at, :] = total


class RingScatter:
    def __init__(self, sender, base, ring, block, relayed, arriving):
        self.s, self.base, self.block, self.relayed, self.arriving = sender, base, block, relayed, arriving
        self.me, self.right, self.left = ring
        self.prev, self.next, self.far = around(self.me)

    def start(self):
        self.s.start(self.base, self.block(self.far, 0), self.relayed(0), self.right)
        self.s.start(self.base + 1, self.block(self.far, 1), self.relayed(1), self.left)
        self.s.start(self.base + 2, self.block(self.next, 1), self.arriving(0, 1), self.right)
        self.s.start(self.base + 3, self.block(self.prev, 0), self.arriving(1, 0), self.left)

    def relay(self, to_next, to_prev):
        self.s.arrived(self.base, self.relayed(0), self.left)
        add_into(self.relayed(0), to_next)
        self.s.start(self.base + 4, self.relayed(0), self.arriving(0, 0), self.right)
        self.s.arrived(self.base + 1, self.relayed(1), self.right)
        add_into(self.relayed(1), to_prev)
        self.s.start(self.base + 5, self.relayed(1), self.arriving(1, 1), self.left)

    def finish(self):
        self.s.arrived(self.base + 2, self.arriving(0, 1), self.left)
        self.s.arrived(self.base + 3, self.arriving(1, 0), self.right)
        self.s.arrived(self.base + 4, self.arriving(0, 0), self.left)
        self.s.arrived(self.base + 5, self.arriving(1, 1), self.right)


class GradScatter:
    def __init__(self, p, sender, base, up, down, bufs, sems):
        self.p, self.sems, self.up, self.down = p, sems, up, down
        (self.u_rel, self.u_arr, self.u_loc, self.u_own, self.u_rel2, self.u_arr2,
         self.d_rel, self.d_arr, self.d_loc, self.d_own, self.d_rel2, self.d_arr2) = bufs
        ring_y, ring_z = p.along("y"), p.along("z")
        half = lambda h: pl.ds(2 * h, 2)
        u_rows, d_rows = up.shape[2] // 2, down.shape[2] // 2
        u_part, d_part = (lambda h: pl.ds(h * u_rows, u_rows)), (lambda h: pl.ds(h * d_rows, d_rows))
        self.up1 = RingScatter(sender, base, ring_y, lambda i, h: up.at[half(h), i], lambda h: self.u_rel.at[h],
                               lambda side, h: self.u_arr.at[side, half(h)])
        self.down1 = RingScatter(sender, base + 6, ring_z, lambda i, h: down.at[i, half(h)], lambda h: self.d_rel.at[h],
                                 lambda side, h: self.d_arr.at[side, half(h)])
        self.up2 = RingScatter(sender, base + 12, ring_z, lambda i, h: self.u_own.at[i, u_part(h)], lambda h: self.u_rel2.at[h],
                               lambda side, h: self.u_arr2.at[side, u_part(h)])
        self.down2 = RingScatter(sender, base + 18, ring_y, lambda i, h: self.d_own.at[i, d_part(h)], lambda h: self.d_rel2.at[h],
                                 lambda side, h: self.d_arr2.at[side, d_part(h)])
        self.u_part, self.d_part = u_part, d_part
        u, d = self.up1, self.down1
        pairs = [(up.at[half(0), u.next], self.u_loc.at[0]), (up.at[half(1), u.prev], self.u_loc.at[1]),
                 (up.at[:, u.me], self.u_own), (down.at[d.next, half(0)], self.d_loc.at[0]),
                 (down.at[d.prev, half(1)], self.d_loc.at[1]), (down.at[d.me], self.d_own)]
        self.loads = [pltpu.make_async_copy(src, dst, sems.at[k]) for k, (src, dst) in enumerate(pairs)]

    def load(self):
        for copy in self.loads:
            copy.start()

    def start(self):
        self.up1.start()
        self.down1.start()

    def relay(self):
        for copy in self.loads:
            copy.wait()
        self.up1.relay(self.u_loc.at[0], self.u_loc.at[1])
        self.down1.relay(self.d_loc.at[0], self.d_loc.at[1])

    def second(self):
        self.up1.finish()
        add_into(self.u_own, self.u_arr.at[0], self.u_arr.at[1])
        self.up2.start()
        self.down1.finish()
        add_into(self.d_own, self.d_arr.at[0], self.d_arr.at[1])
        self.down2.start()
        u, d = self.up2, self.down2
        u.relay(self.u_own.at[u.next, self.u_part(0)], self.u_own.at[u.prev, self.u_part(1)])
        d.relay(self.d_own.at[d.next, self.d_part(0)], self.d_own.at[d.prev, self.d_part(1)])

    def finish(self, up_out, down_out):
        self.up2.finish()
        self.down2.finish()
        up_out[...] = (self.u_own[self.up2.me] + self.u_arr2[0] + self.u_arr2[1]).T
        down_out[...] = self.d_own[self.down2.me] + self.d_arr2[0] + self.d_arr2[1]

    @staticmethod
    def buffers(up, down):
        f32 = jnp.float32
        out = []
        for rows, cols in (up.shape[2:], down.shape[2:]):
            out += [(2, 2, rows, cols), (2, RING, rows, cols), (2, 2, rows, cols), (RING, rows, cols),
                    (2, rows // 2, cols), (2, rows, cols)]
        return [pltpu.VMEM(shape, f32) for shape in out]


def scatter_kernel(h_ref, w_ref, *refs):
    p = Place()
    me, right, left = p.along("x")
    sib, c, o = p.sibling(), p.core, 1 - p.core
    (g_up, g_down, x_ref, c_ref, dx_ref, up_out, down_out, y_ref, to_sib, from_sib, acc, relayed, arriving, send_sems, recv_sems,
     up_sum, local_sems, *bufs) = refs
    ring_y, ring_z = p.along("y"), p.along("z")
    turns = p.turns()
    greet([p.dev(x=x, core=core) for x, core in turns] + [ring_y[1], ring_y[2], ring_z[1], ring_z[2]])
    s = Sender(send_sems, recv_sems)
    grads = GradScatter(p, s, 10, g_up, g_down, bufs, local_sems)
    grads.start()
    grads.load()
    hidden = y_ref.shape[1]
    rows = y_ref.shape[0] // 2
    first, second = pl.ds(0, rows), pl.ds(rows, rows)

    def product(dx, core, dst, part=slice(None)):
        block = lax.rem(me + dx, RING)

        @pl.loop(0, hidden // STEP)
        def _(n):
            at = slab(n, STEP)
            dst[:, at] = lax.dot_general(h_ref[block, core, part, :], w_ref[at, :], ROWS,
                                         preferred_element_type=jnp.float32)

    def both(k, dx, dst):
        product(dx, o, to_sib.at[k])
        s.start(k, to_sib.at[k], from_sib.at[k], sib)
        product(dx, c, dst)

    def joined(k, dst):
        s.arrived(k, from_sib.at[k], sib)
        add_into(dst, from_sib.at[k])

    parts = ((first, right, 0), (second, left, GRAD_SLOTS - 1))
    for h, (part, _, slot) in enumerate(parts):
        product(2, o, to_sib.at[0, part], part)
        s.start(slot, to_sib.at[0, part], from_sib.at[0, part], sib)
    for h, (part, to, slot) in enumerate(parts):
        product(2, c, acc.at[0, part], part)
        s.arrived(slot, from_sib.at[0, part], sib)
        add_into(acc.at[0, part], from_sib.at[0, part])
        s.start(4 + h, acc.at[0, part], relayed.at[h], to)
    both(1, 1, acc.at[1])
    both(2, 3, acc.at[2])
    joined(1, acc.at[1])
    s.start(6, acc.at[1, second], arriving.at[0, second], right)
    joined(2, acc.at[2])
    s.start(7, acc.at[2, first], arriving.at[1, first], left)
    both(3, 0, y_ref)
    joined(3, y_ref)
    grads.relay()
    s.arrived(4, relayed.at[0], left)
    add_into(acc.at[1, first], relayed.at[0])
    s.start(8, acc.at[1, first], arriving.at[0, first], right)
    s.arrived(5, relayed.at[1], right)
    add_into(acc.at[2, second], relayed.at[1])
    s.start(9, acc.at[2, second], arriving.at[1, second], left)
    grads.second()
    grads.finish(up_sum, down_out)
    mine = me * CORES + c
    piece = up_out.shape[1]
    keep = pltpu.make_async_copy(up_sum.at[slab(mine, piece)], up_out.at[mine], local_sems.at[6])
    keep.start()
    for k, (x, core) in enumerate(turns):
        to = x * CORES + core
        s.start(GRAD_SLOTS + k, up_sum.at[slab(to, piece)], up_out.at[mine], p.dev(x=x, core=core))
    s.arrived(6, arriving.at[0, second], left)
    s.arrived(7, arriving.at[1, first], right)
    s.arrived(8, arriving.at[0, first], left)
    s.arrived(9, arriving.at[1, second], right)
    for h in HALVES:
        @pl.loop(0, rows // NORM_ROWS)
        def _(r):
            at = slab(r, NORM_ROWS)
            there = pl.ds(pl.multiple_of(h * rows + r * NORM_ROWS, NORM_ROWS), NORM_ROWS)
            v = y_ref[there, :] + arriving[0, there, :] + arriving[1, there, :]
            pull = jax.vjp(norm_f32, x_ref[h, at, :].astype(jnp.float32))[1]
            dx_ref[h, at, :] = (c_ref[h, at, :].astype(jnp.float32) + pull(v)[0]).astype(jnp.bfloat16)

    for k, (x, core) in enumerate(p.turns(-1)):
        s.arrived(GRAD_SLOTS + k, up_out.at[x * CORES + core], p.dev(x=x, core=core))
    keep.wait()
    s.drain()


def scatter(h, w, grads, x, c):
    rows, width = h.shape[2:]
    hidden = w.shape[0]
    vmem, anywhere = pl.BlockSpec(memory_space=pltpu.VMEM), pl.BlockSpec(memory_space=pl.ANY)
    f32 = jnp.float32
    up_rows, down_rows = grads[0].shape[3], grads[1].shape[2]
    n_data = RING * CORES
    slots = GRAD_SLOTS + n_data
    return pl.pallas_call(
        scatter_kernel,
        out_shape=[jax.ShapeDtypeStruct(x.shape, x.dtype),
                   jax.ShapeDtypeStruct((n_data, up_rows // n_data, width), f32), jax.ShapeDtypeStruct((down_rows, hidden), f32)],
        in_specs=[vmem] * 2 + [anywhere] * 2 + [vmem] * 2,
        out_specs=[vmem] * 3,
        scratch_shapes=[pltpu.VMEM((rows, hidden), f32), pltpu.VMEM((RING, rows, hidden), f32), pltpu.VMEM((RING, rows, hidden), f32),
                        pltpu.VMEM((3, rows, hidden), f32), pltpu.VMEM((2, rows // 2, hidden), f32),
                        pltpu.VMEM((2, rows, hidden), f32),
                        pltpu.SemaphoreType.DMA((slots,)), pltpu.SemaphoreType.DMA((slots,)),
                        pltpu.VMEM((up_rows, width), f32), pltpu.SemaphoreType.DMA((7,))] + GradScatter.buffers(*grads),
        compiler_params=pltpu.CompilerParams(collective_id=2, has_side_effects=True, vmem_limit_bytes=VMEM),
        name="scatter_grads",
    )(h, w, *grads, x, c)


def solution(mesh):
    n_data = mesh.shape["data"]
    n_local = mesh.shape["local"]

    def body(tokens, cotangent, w_up, w_down):
        micro, rows, hidden = tokens.shape
        layers, up_rows, ffn = w_up.shape
        down_rows = w_down.shape[1]
        pad = PAD - down_rows
        width = n_local * PAD
        own = micro * rows

        up = w_up.reshape(layers, up_rows, n_local, n_data, down_rows)
        up = jnp.pad(up, ((0, 0),) * 4 + ((0, pad),))
        up = up.transpose(3, 0, 1, 2, 4).reshape(n_data, layers, up_rows, width)
        down = jnp.pad(w_down, ((0, 0), (0, pad), (0, 0)))

        def blocks(h):
            return h.reshape(RING, CORES, own, width)

        x_cur = tokens
        saved = []
        for layer in range(layers):
            u_all, slope, act, x_next, *ups = forward(x_cur, up if layer == 0 else up[layer], down[layer], layer == 0)
            if ups:
                up, = ups
            saved.append((x_cur, u_all, slope, act))
            x_cur = x_next
        x_final = x_cur

        d_cur, x_final = lax.optimization_barrier((cotangent, x_final))
        grads_up = [None] * layers
        grads_down = [None] * layers
        for layer in reversed(range(layers)):
            x_in, u_all, slope, act = saved[layer]
            z, w1, g_up, g_down = gather_back(d_cur, up[layer], down[layer], u_all, slope, act)
            d_cur, grads_up[layer], g_down = scatter(blocks(z), w1.reshape(hidden, width), (g_up, g_down), x_in, d_cur)
            grads_down[layer] = g_down[:down_rows]
        g_up = jnp.stack(grads_up, 1).reshape(n_data, layers, up_rows, n_local, PAD)[..., :down_rows]
        g_up = g_up.transpose(1, 2, 3, 0, 4).reshape(layers, up_rows, ffn)
        return x_final, d_cur, g_up, jnp.stack(grads_down)

    spec = P(None, ALL_AXES, None)
    return jax.shard_map(body, mesh=mesh, in_specs=(spec,) * 4, out_specs=(spec,) * 4, check_vma=False)
```
